256 devices in a mesh: blk: 128 (over z_lo, y, x, core), rep: 2 (over z_hi).
Axes of the slice: x: 4, y: 4, z: 8 (z_hi: 2, z_lo: 4; z = z_hi * 4 + z_lo), core: 2. Of those that a mesh axis runs over, the one named last changes fastest.
Arguments:
- load_coef: bfloat16 [256, 2049, 256], P('blk', None, 'rep'), parts along dimension 2, may hold values from -0.29882812 to 0.29882812
- legendre: bfloat16 [256, 2049, 1024], P('blk'), may hold values from -0.125 to 0.125
- slab_orders: int32 [256], replicated, may hold values from 0 to 1023, as said below
- cycle_rows: int32 [1024], replicated, may hold values from 0 to 1023, each once
Outputs:
- potential: bfloat16 [1024, 128, 4096], P('blk', 'rep'), parts along dimension 1
- energy: float32 [128], P('rep'), parts along dimension 0
The draws below stay inside these ranges and needn't reach their ends.
There are 2 independent parts, one for each index of `rep`. The reference program is written for one: setup_inputs(seed, part) draws one part's arguments, and reference() takes and returns one part's arrays. A program takes and returns all parts, laid end to end along the dimension named above; an argument that names none is the same for every part. Nothing has to cross between parts.
Inputs may be any that keep to these rules, and one draw needn't show every extreme that they name: `slab_orders`: values are distinct and below (2048) / 2. `cycle_rows`: each cycle appears once.
All inputs are finite; a program needn't handle non-finite values.
Results may differ from the reference program's by a relative error of at most 0.0055.
Values may be sent and summed in bfloat16 or wider, within the bound.
No kernel may reach another device: no remote copies, remote signals or barrier semaphores. Data moves between devices by JAX's collectives and lax.ppermute only.
A program may use at most 128 MiB of HBM per device.

```python
import math
import jax
import jax.numpy as jnp
from jax import lax

DEGREE = 2047
NLAT = 1024
NLON = 4096
FIELDS = 64
SLAB = 2049
PAIRS = 256


def draw_slab_orders(key, part):
    return jax.random.permutation(key, (DEGREE + 1) // 2)[:PAIRS].astype(jnp.int32)


def levels(key, dims, shards, smallest, top_value):
    loudness = 1.0
    for axis_at, blocks in shards:
        draws = jax.random.uniform(jax.random.fold_in(jax.random.fold_in(key, 6), axis_at), (blocks,), jnp.float32, smallest / len(shards), top_value / len(shards))
        loudness = loudness * jnp.repeat(jnp.exp(draws), dims[axis_at] // blocks).reshape((-1,) + (1,) * (len(dims) - 1 - axis_at))
    return loudness


def scatter_about(key, dims, scale, limit, pieces=(), kind=jnp.bfloat16):
    values = jax.random.normal(key, dims, jnp.float32) * scale
    if len(pieces) > 0:
        values = levels(key, dims, pieces, -0.22, 0.18) * values
    return jnp.clip(values, min=-limit, max=limit).astype(kind)


def setup_inputs(seed: int = 0, part: int = 0) -> dict:
    streams_of = jax.random.split(jax.random.key(seed), 5)
    part_splits = jax.random.split(jax.random.fold_in(streams_of[4], part), 5)
    load_coef = scatter_about(part_splits[0], (PAIRS, SLAB, 2 * FIELDS), 0.05, 0.29882812, ((0, 128),))
    legendre = scatter_about(streams_of[1], (PAIRS, SLAB, NLAT), SLAB ** -0.5, 0.125, ((0, 128),))
    slab_orders = draw_slab_orders(jax.random.fold_in(streams_of[4], 71), part)
    cycle_rows = jax.random.permutation(streams_of[3], NLAT).astype(jnp.int32)
    return {"load_coef": load_coef, "legendre": legendre, "slab_orders": slab_orders, "cycle_rows": cycle_rows}


def basis_table(orders):
    longitude_ids = jnp.arange(NLON, dtype=jnp.int32)
    phase_ids = (orders[:, None] * longitude_ids[None, :]) % NLON
    angles = phase_ids.astype(jnp.float32) * (2.0 * math.pi / NLON)
    factor = jnp.where(orders == 0, 1.0, 2.0).astype(jnp.float32)[:, None]
    return (factor * jnp.cos(angles)).astype(jnp.bfloat16), (-factor * jnp.sin(angles)).astype(jnp.bfloat16)


def reference(load_coef, legendre, slab_orders, cycle_rows):
    slab_rows = DEGREE + 2
    row_ids = jnp.arange(slab_rows, dtype=jnp.int32)

    def synthesize(pair_args):
        pair_coef, pair_table, low_order = pair_args
        in_lower = (row_ids < slab_rows - 1 - low_order)[:, None]
        nothing = jnp.zeros_like(pair_coef)
        stacked = jnp.concatenate([jnp.where(in_lower, pair_coef, nothing), jnp.where(in_lower, nothing, pair_coef)], axis=1)
        return lax.dot_general(stacked, pair_table, (((0,), (0,)), ((), ())), preferred_element_type=jnp.float32).astype(jnp.bfloat16)

    spectra = lax.map(synthesize, (load_coef, legendre, slab_orders))
    spectra = spectra.reshape(PAIRS, 4, FIELDS, NLAT)
    cos_lower, sin_lower = basis_table(slab_orders.astype(jnp.int32))
    cos_upper, sin_upper = basis_table((DEGREE - slab_orders).astype(jnp.int32))
    basis = jnp.stack([cos_lower, sin_lower, cos_upper, sin_upper], axis=1).reshape(PAIRS * 4, NLON)

    def per_field(field_index):
        rows = spectra[:, :, field_index, :].reshape(PAIRS * 4, NLAT)
        wave = lax.dot_general(rows, basis, (((0,), (0,)), ((), ())), preferred_element_type=jnp.float32)
        energy = jnp.sum(wave * wave) / (NLAT * NLON)
        return wave[cycle_rows].astype(jnp.bfloat16), energy

    potential, energy = lax.map(per_field, jnp.arange(FIELDS, dtype=jnp.int32))
    return jnp.transpose(potential, (1, 0, 2)), energy
```

```python
import functools
import math

import jax
import jax.numpy as jnp
from jax import lax
from jax.experimental import pallas as pl
from jax.experimental.pallas import tpu as pltpu
from jax.sharding import Mesh
from jax.sharding import PartitionSpec as P

NLON = 4096
HALF = NLON // 2
BLK = ("blk_0", "blk_1", "blk_2", "blk_3")
ROWS = 512
TILE = 512


def spectra_body(orders, cycles, coef, table, out, energy, onehot, acc, *, slab_rows, steps, blocks):
    pair, step = pl.program_id(0), pl.program_id(1)
    fields2 = coef.shape[2]
    lat = table.shape[2]
    low = orders[lax.axis_index(BLK) * pl.num_programs(0) + pair]
    cut = slab_rows - 1 - low
    low_is_even = low % 2 == 0

    @pl.when((pair == 0) & (step == 0))
    def _():
        energy[...] = jnp.zeros_like(energy)
        for at in range(0, lat, 128):
            row = jnp.broadcast_to(cycles[:, at : at + 128], (128, 128))
            column = row.T
            for j in range(0, lat, 128):
                lane = lax.broadcasted_iota(jnp.int32, (128, 128), 1) + j
                onehot[at : at + 128, j : j + 128] = (column == lane).astype(jnp.float32).astype(jnp.bfloat16)

    def product(count, rows):
        turned = coef[0, :count, :].astype(jnp.float32).T
        ids = step * ROWS + lax.broadcasted_iota(jnp.int32, turned.shape, 1)
        in_low = ids < cut
        inside = ids < slab_rows
        even = in_low == low_is_even
        zero = jnp.zeros_like(turned)
        left = jnp.concatenate(
            [jnp.where(inside & even, turned, zero), jnp.where(inside & ~even, turned, zero)], axis=0
        ).astype(jnp.bfloat16)
        return jnp.dot(left, rows, preferred_element_type=jnp.float32)

    @pl.when(step == 0)
    def _():
        acc[...] = product(ROWS, table[0])

    @pl.when((step > 0) & (step < steps - 1))
    def _():
        acc[...] += product(ROWS, table[0])

    @pl.when(step == steps - 1)
    def _():
        rest = table[0, :128, :].astype(jnp.float32)
        ids = step * ROWS + lax.broadcasted_iota(jnp.int32, rest.shape, 0)
        rest = jnp.where(ids < slab_rows, rest, 0.0).astype(jnp.bfloat16)
        spectrum = (acc[...] + product(128, rest)).astype(jnp.bfloat16)
        moved = lax.dot_general(
            onehot[...], spectrum, (((1,), (1,)), ((), ())), preferred_element_type=jnp.float32
        )
        out[:, pl.ds(pl.multiple_of(pair * 2 * fields2, 2 * fields2), 2 * fields2)] = moved.astype(jnp.bfloat16)
        wide = spectrum.astype(jnp.float32)
        squares = wide * wide
        part = squares[:, :128]
        for j in range(128, lat, 128):
            part = part + squares[:, j : j + 128]
        sums = jnp.sum(part.T, axis=0, keepdims=True)
        lane = lax.broadcasted_iota(jnp.int32, (1, fields2), 1)
        real = lane < fields2 // 2
        zero_weight = jnp.where(real, 1.0, 0.0)
        weight = jnp.where(low == 0, zero_weight, 2.0)
        scale = NLON / (lat * NLON)
        both = sums[:, :fields2] * (weight * scale) + sums[:, fields2:] * (2.0 * scale)
        both = both + pltpu.roll(both, fields2 // 2, 1)
        energy[...] += jnp.broadcast_to(both, energy.shape)


def spectra_of(load_coef, legendre, slab_orders, cycle_rows, blocks):
    pairs, slab_rows, fields2 = load_coef.shape
    lat = legendre.shape[2]
    steps = pl.cdiv(slab_rows, ROWS)
    return pl.pallas_call(
        functools.partial(spectra_body, slab_rows=slab_rows, steps=steps, blocks=blocks),
        grid_spec=pltpu.PrefetchScalarGridSpec(
            num_scalar_prefetch=1,
            grid=(pairs, steps),
            in_specs=[
                pl.BlockSpec((1, lat), lambda p, s, o: (0, 0)),
                pl.BlockSpec((1, ROWS, fields2), lambda p, s, o: (p, s, 0)),
                pl.BlockSpec((1, ROWS, lat), lambda p, s, o: (p, s, 0)),
            ],
            out_specs=[
                pl.BlockSpec((lat, pairs * 2 * fields2), lambda p, s, o: (0, 0)),
                pl.BlockSpec((blocks, fields2), lambda p, s, o: (0, 0)),
            ],
            scratch_shapes=[
                pltpu.VMEM((lat, lat), jnp.bfloat16),
                pltpu.VMEM((2 * fields2, lat), jnp.float32),
            ],
        ),
        out_shape=[
            jax.ShapeDtypeStruct((lat, pairs * 2 * fields2), jnp.bfloat16),
            jax.ShapeDtypeStruct((blocks, fields2), jnp.float32),
        ],
        compiler_params=pltpu.CompilerParams(dimension_semantics=("arbitrary", "arbitrary")),
        name="spectra",
    )(slab_orders, cycle_rows.reshape(1, lat), load_coef, legendre)


def basis_body(orders, even_out, odd_out, columns, *, pairs, blocks, degree):
    count = pairs * blocks
    columns[...] = jnp.broadcast_to(orders[...], (128, count)).T
    lane = lax.broadcasted_iota(jnp.int32, (blocks, 128), 1)
    scale = 2.0 * math.pi / NLON
    for pair in range(pairs):
        low = columns[pl.ds(pair, blocks, stride=pairs), :]
        high = degree - low
        is_even = low % 2 == 0
        for out, order in ((even_out, jnp.where(is_even, low, high)), (odd_out, jnp.where(is_even, high, low))):
            fine = (order * lane % NLON).astype(jnp.float32) * scale
            turn = (order * 128 % NLON).astype(jnp.float32) * scale
            factor = jnp.where(order == 0, 1.0, 2.0)
            cosine, sine = factor * jnp.cos(fine), -factor * jnp.sin(fine)
            turn_cos, turn_sin = jnp.cos(turn), jnp.sin(turn)
            for at in range(0, HALF, 128):
                out[pl.ds(2 * pair * blocks, blocks), at : at + 128] = cosine.astype(jnp.bfloat16)
                out[pl.ds((2 * pair + 1) * blocks, blocks), at : at + 128] = sine.astype(jnp.bfloat16)
                cosine, sine = cosine * turn_cos + sine * turn_sin, sine * turn_cos - cosine * turn_sin


def basis_of(slab_orders, pairs, blocks, degree):
    shape = jax.ShapeDtypeStruct((2 * pairs * blocks, HALF), jnp.bfloat16)
    return pl.pallas_call(
        functools.partial(basis_body, pairs=pairs, blocks=blocks, degree=degree),
        out_shape=[shape, shape],
        scratch_shapes=[pltpu.VMEM((pairs * blocks, 128), jnp.int32)],
        name="basis",
    )(slab_orders.reshape(1, pairs * blocks))


def wave_body(received, even_basis, odd_basis, out, wide, even_left, odd_left, staged, sems, *, pairs, blocks, rows, fields):
    step = pl.program_id(0)

    @pl.when(step == 0)
    def _():
        for pair in range(pairs):
            for parity, left in enumerate((even_left, odd_left)):
                group = pair * 2 + parity
                wide[group] = received[:, group * 128 : (group + 1) * 128].astype(jnp.float32)
                for row in range(rows):
                    turned = wide[group, pl.ds(row, blocks, stride=rows), :].T.astype(jnp.bfloat16)
                    for part in range(2):
                        to = (pair * 2 + part) * blocks
                        left[row * fields : (row + 1) * fields, to : to + blocks] = turned[part * fields : (part + 1) * fields, :]

    even = jnp.dot(even_left[...], even_basis[...], preferred_element_type=jnp.float32)
    odd = jnp.dot(odd_left[...], odd_basis[...], preferred_element_type=jnp.float32)
    shape = (rows, fields, TILE)
    for half, value in enumerate((even + odd, even - odd)):
        at = pl.multiple_of(half * HALF + step * TILE, TILE)
        staged[:, :, pl.ds(at, TILE)] = value.astype(jnp.bfloat16).reshape(shape)
        pltpu.make_async_copy(
            staged.at[:, :, pl.ds(at, TILE)], out.at[:, :, pl.ds(at, TILE)], sems.at[half, step]
        ).start()

    @pl.when(step == pl.num_programs(0) - 1)
    def _():
        for half in range(2):
            for tile in range(HALF // TILE):
                at = half * HALF + tile * TILE
                pltpu.make_async_copy(
                    staged.at[:, :, at : at + TILE], out.at[:, :, at : at + TILE], sems.at[half, tile]
                ).wait()


def wave_of(received, even_basis, odd_basis, pairs, blocks, rows, fields):
    depth = 2 * pairs * blocks
    return pl.pallas_call(
        functools.partial(wave_body, pairs=pairs, blocks=blocks, rows=rows, fields=fields),
        grid=(HALF // TILE,),
        in_specs=[
            pl.BlockSpec(received.shape, lambda t: (0, 0)),
            pl.BlockSpec((depth, TILE), lambda t: (0, t)),
            pl.BlockSpec((depth, TILE), lambda t: (0, t)),
        ],
        out_specs=pl.BlockSpec(memory_space=pl.ANY),
        out_shape=jax.ShapeDtypeStruct((rows, fields, NLON), jnp.bfloat16),
        scratch_shapes=[
            pltpu.VMEM((2 * pairs, received.shape[0], 2 * fields), jnp.float32),
            pltpu.VMEM((rows * fields, depth), jnp.bfloat16),
            pltpu.VMEM((rows * fields, depth), jnp.bfloat16),
            pltpu.VMEM((rows, fields, NLON), jnp.bfloat16),
            pltpu.SemaphoreType.DMA((2, HALF // TILE)),
        ],
        compiler_params=pltpu.CompilerParams(dimension_semantics=("arbitrary",)),
        name="wave",
    )(received, even_basis, odd_basis)


def shards(load_coef, legendre, slab_orders, cycle_rows):
    blocks = lax.axis_size(BLK)
    pairs, slab_rows, fields2 = load_coef.shape
    lat = legendre.shape[2]
    rows = lat // blocks
    spectra, energy = spectra_of(load_coef, legendre, slab_orders, cycle_rows, blocks)
    received = lax.all_to_all(spectra.reshape(blocks, rows, -1), BLK, split_axis=0, concat_axis=0, tiled=True)
    even_basis, odd_basis = basis_of(slab_orders, pairs, blocks, slab_rows - 2)
    shared = lax.all_to_all(energy.reshape(blocks, 1, fields2), BLK, split_axis=0, concat_axis=0, tiled=True)
    energy = jnp.sum(shared, axis=(0, 1))[: fields2 // 2]
    wave = wave_of(received.reshape(lat, -1), even_basis, odd_basis, pairs, blocks, rows, fields2 // 2)
    return wave, energy


def solution(mesh):
    split = Mesh(
        mesh.devices.reshape(4, 4, 4, 2, mesh.shape["rep"]),
        ("blk_0", "blk_1", "blk_2", "blk_3", "rep"),
    )
    in_specs = (P(BLK, None, "rep"), P(BLK, None, None), P(), P())
    out_specs = (P(BLK, "rep", None), P("rep"))
    return jax.shard_map(
        shards, mesh=split, in_specs=in_specs, out_specs=out_specs, check_vma=False
    )
```

```python
import functools
import math

import jax
import jax.numpy as jnp
from jax import lax
from jax.experimental import pallas as pl
from jax.experimental.pallas import tpu as pltpu
from jax.sharding import Mesh
from jax.sharding import PartitionSpec as P


NLON = 4096
HALF = NLON // 2
BLK = ("blk_0", "blk_1", "blk_2", "blk_3")
DEPTH = 512
TILE = 256


def spectra_body(orders, cycles, coef_hbm, table_hbm, out, coef, table, tail, low_sum, high_sum, moved_out, energy_out, sems, *, slab_rows, depth):
    pairs, fields2 = coef_hbm.shape[1], coef_hbm.shape[2]
    lat = table_hbm.shape[2]
    chunks = slab_rows // depth
    whole = chunks * depth
    columns = lat // 128

    def piece(chunk, column):
        return pltpu.make_async_copy(
            table_hbm.at[pl.ds(chunk * depth, depth), :, pl.ds(column * 128, 128)],
            table.at[chunk, column],
            sems.at[chunk, column],
        )

    def last(column):
        return pltpu.make_async_copy(
            table_hbm.at[pl.ds(whole, 1), :, pl.ds(column * 128, 128)],
            tail.at[column, pl.ds(0, 1)],
            sems.at[chunks, column],
        )

    coef_copy = pltpu.make_async_copy(coef_hbm, coef.at[pl.ds(0, slab_rows)], sems.at[chunks + 1, 0])
    coef_copy.start()
    for column in range(columns):
        piece(0, column).start()
    for column in range(columns):
        last(column).start()
    for chunk in range(1, chunks):
        for column in range(columns):
            piece(chunk, column).start()

    first = lax.axis_index(BLK) * pairs
    lows = [orders[first + pair] for pair in range(pairs)]
    coef_copy.wait()
    flat = coef.reshape(coef.shape[0] * pairs, fields2)

    def left_of(start, count, side):
        turned = flat[start * pairs : (start + count) * pairs, :].astype(jnp.float32).T
        lane = lax.broadcasted_iota(jnp.int32, turned.shape, 1)
        parts = []
        for pair in range(pairs):
            mine = lane % pairs == pair
            row = start + lane // pairs
            if side == "low":
                mine = mine & (row < slab_rows - 1 - lows[pair])
            elif side == "high":
                mine = mine & (row >= slab_rows - 1 - lows[pair]) & (row < slab_rows)
            parts.append(jnp.where(mine, turned, 0.0))
        return jnp.concatenate(parts, axis=0).astype(jnp.bfloat16)

    for column in range(columns):
        last(column).wait()
    ends = []
    for column in range(columns):
        end = tail.at[column].reshape(tail.shape[1] * pairs, 128)[...].astype(jnp.float32)
        keep = lax.broadcasted_iota(jnp.int32, end.shape, 0) < pairs
        ends.append(jnp.where(keep, end, 0.0).astype(jnp.bfloat16))
    ends = jnp.concatenate(ends, axis=1)
    high_sum[...] = jnp.dot(left_of(whole, tail.shape[1], "high"), ends, preferred_element_type=jnp.float32)

    for chunk in range(chunks):
        start = chunk * depth
        sure = start + depth <= slab_rows // 2
        low_left = left_of(start, depth, None if sure else "low")
        high_left = None if sure else left_of(start, depth, "high")
        for column in range(columns):
            piece(chunk, column).wait()
        right = jnp.concatenate(
            [table.at[chunk, column].reshape(depth * pairs, 128)[...] for column in range(columns)], axis=1
        )
        low = jnp.dot(low_left, right, preferred_element_type=jnp.float32)
        low_sum[...] = low if chunk == 0 else low_sum[...] + low
        if not sure:
            high_sum[...] += jnp.dot(high_left, right, preferred_element_type=jnp.float32)

    spectrum = []
    for pair in range(pairs):
        even = lows[pair] % 2 == 0
        low = low_sum[pair * fields2 : (pair + 1) * fields2, :]
        high = high_sum[pair * fields2 : (pair + 1) * fields2, :]
        spectrum.append(jnp.where(even, low, high).astype(jnp.bfloat16))
        spectrum.append(jnp.where(even, high, low).astype(jnp.bfloat16))
    spectrum = jnp.concatenate(spectrum, axis=0)

    lane = lax.broadcasted_iota(jnp.int32, (128, lat), 1)
    onehot = []
    for at in range(0, lat, 128):
        column = jnp.broadcast_to(cycles[:, at : at + 128], (128, 128)).T
        column = jnp.concatenate([column] * columns, axis=1)
        onehot.append((column == lane).astype(jnp.float32).astype(jnp.bfloat16))
    onehot = jnp.concatenate(onehot, axis=0)
    moved = lax.dot_general(onehot, spectrum, (((1,), (1,)), ((), ())), preferred_element_type=jnp.float32)
    groups = moved_out.shape[0]
    tiles = moved_out.shape[2]
    copies = []
    for group in range(groups):
        part = moved[:, group * fields2 : (group + 1) * fields2].astype(jnp.bfloat16)
        moved_out.at[group].reshape(lat, fields2)[...] = part
        copies.append(
            pltpu.make_async_copy(
                moved_out.at[group], out.at[:, pl.ds(group * tiles, tiles)], sems.at[chunks + 1, 1 + group]
            )
        )
        copies[-1].start()

    sums = jnp.sum(moved * moved, axis=0, keepdims=True)
    lane = lax.broadcasted_iota(jnp.int32, (1, fields2), 1)
    real = lane < fields2 // 2
    total = jnp.zeros((1, fields2), jnp.float32)
    for pair in range(pairs):
        weight = jnp.where(lows[pair] == 0, jnp.where(real, 1.0, 0.0), 2.0)
        at = 2 * pair * fields2
        total = total + sums[:, at : at + fields2] * weight + sums[:, at + fields2 : at + 2 * fields2] * 2.0
    total = (total + pltpu.roll(total, fields2 // 2, 1)) * (1.0 / lat)
    top = total.astype(jnp.bfloat16).astype(jnp.float32)
    middle = (total - top).astype(jnp.bfloat16).astype(jnp.float32)
    bottom = total - top - middle
    blocks = energy_out.shape[0]
    odd_row = lax.broadcasted_iota(jnp.int32, (2 * blocks, fields2), 0) % 2 == 1
    first_row = jnp.broadcast_to(jnp.where(real, top, middle), odd_row.shape)
    second_row = jnp.broadcast_to(jnp.where(real, bottom, 0.0), odd_row.shape)
    energy_out.reshape(2 * blocks, fields2)[...] = jnp.where(odd_row, second_row, first_row).astype(jnp.bfloat16)
    copies.append(
        pltpu.make_async_copy(energy_out, out.at[:, groups * tiles], sems.at[chunks + 1, 1 + groups])
    )
    copies[-1].start()
    for copy in copies:
        copy.wait()


def spectra_of(load_coef, legendre, slab_orders, cycle_rows, blocks):
    pairs, slab_rows, fields2 = load_coef.shape
    lat = legendre.shape[2]
    columns = lat // 128
    chunks = slab_rows // DEPTH
    tiles = lat // blocks // 2
    anywhere = pl.BlockSpec(memory_space=pltpu.HBM)
    vmem = pl.BlockSpec(memory_space=pltpu.VMEM)
    return pl.pallas_call(
        functools.partial(spectra_body, slab_rows=slab_rows, depth=DEPTH),
        in_specs=[pl.BlockSpec(memory_space=pltpu.SMEM), vmem, anywhere, anywhere],
        out_specs=anywhere,
        out_shape=jax.ShapeDtypeStruct((blocks, pairs * 2 * tiles + 1, 2, fields2), jnp.bfloat16),
        scratch_shapes=[
            pltpu.VMEM((slab_rows // 64 * 64 + 64, pairs, fields2), jnp.bfloat16),
            pltpu.VMEM((chunks, columns, DEPTH, pairs, 128), jnp.bfloat16),
            pltpu.VMEM((columns, 64, pairs, 128), jnp.bfloat16),
            pltpu.VMEM((pairs * fields2, lat), jnp.float32),
            pltpu.VMEM((pairs * fields2, lat), jnp.float32),
            pltpu.VMEM((pairs * 2, blocks, tiles, 2, fields2), jnp.bfloat16),
            pltpu.VMEM((blocks, 2, fields2), jnp.bfloat16),
            pltpu.SemaphoreType.DMA((chunks + 2, columns)),
        ],
        compiler_params=pltpu.CompilerParams(vmem_limit_bytes=60 * 2**20),
        name="spectra",
    )(slab_orders, cycle_rows.reshape(1, lat), jnp.transpose(load_coef, (1, 0, 2)), jnp.transpose(legendre, (1, 0, 2)))


def basis_body(orders, out, columns, *, pairs, blocks, degree):
    count = pairs * blocks
    columns[...] = jnp.broadcast_to(orders[...], (128, count)).T
    lane = lax.broadcasted_iota(jnp.int32, (blocks, 128), 1)
    scale = 2.0 * math.pi / NLON
    for pair in range(pairs):
        low = columns[pl.ds(pair, blocks, stride=pairs), :]
        high = degree - low
        is_even = low % 2 == 0
        for parity, order in enumerate((jnp.where(is_even, low, high), jnp.where(is_even, high, low))):
            fine = (order * lane % NLON).astype(jnp.float32) * scale
            turn = (order * 128 % NLON).astype(jnp.float32) * scale
            factor = jnp.where(order == 0, 1.0, 2.0)
            cosine, sine = factor * jnp.cos(fine), -factor * jnp.sin(fine)
            turn_cos, turn_sin = jnp.cos(turn), jnp.sin(turn)
            for at in range(0, HALF, 128):
                out[parity, pl.ds(2 * pair * blocks, blocks), at : at + 128] = cosine.astype(jnp.bfloat16)
                out[parity, pl.ds((2 * pair + 1) * blocks, blocks), at : at + 128] = sine.astype(jnp.bfloat16)
                cosine, sine = cosine * turn_cos + sine * turn_sin, sine * turn_cos - cosine * turn_sin


def basis_of(slab_orders, pairs, blocks, degree):
    shape = jax.ShapeDtypeStruct((2, 2 * pairs * blocks, HALF), jnp.bfloat16)
    return pl.pallas_call(
        functools.partial(basis_body, pairs=pairs, blocks=blocks, degree=degree),
        in_specs=[pl.BlockSpec(memory_space=pltpu.VMEM)],
        out_specs=pl.BlockSpec(memory_space=pltpu.VMEM),
        out_shape=shape,
        scratch_shapes=[pltpu.VMEM((pairs * blocks, 128), jnp.int32)],
        compiler_params=pltpu.CompilerParams(vmem_limit_bytes=12 * 2**20),
        name="basis",
    )(slab_orders.reshape(1, pairs * blocks))


def wave_body(received, basis_hbm, out, energy, wide, even_left, odd_left, basis, staged, sems, *, pairs, blocks, rows, fields):
    stride = wide.shape[0] // blocks

    def fetch(tile):
        return pltpu.make_async_copy(
            basis_hbm.at[:, :, pl.ds(tile * TILE, TILE)], basis.at[tile], sems.at[2, tile]
        )

    for tile in range(HALF // TILE):
        fetch(tile).start()
    wide[...] = received.reshape(*wide.shape)[...].astype(jnp.float32)
    for pair in range(pairs):
        for parity, left in enumerate((even_left, odd_left)):
            for row in range(rows):
                at = (pair * 2 + parity) * rows + row
                turned = wide[pl.ds(at, blocks, stride=stride), :].T.astype(jnp.bfloat16)
                for part in range(2):
                    to = (pair * 2 + part) * blocks
                    left[row * fields : (row + 1) * fields, to : to + blocks] = turned[part * fields : (part + 1) * fields, :]

    at = 2 * pairs * rows
    parts = wide[pl.ds(at, blocks, stride=stride), :] + wide[pl.ds(at + 1, blocks, stride=stride), :]
    total = jnp.sum(parts, axis=0, keepdims=True)
    energy[...] = (total + pltpu.roll(total, fields, 1))[:, :fields]

    def copy(half, tile):
        at = half * HALF + tile * TILE
        return pltpu.make_async_copy(
            staged.at[:, :, pl.ds(at, TILE)], out.at[:, :, pl.ds(at, TILE)], sems.at[half, tile]
        )

    for tile in range(HALF // TILE):
        at = tile * TILE
        fetch(tile).wait()
        even = jnp.dot(even_left[...], basis[tile, 0], preferred_element_type=jnp.float32)
        odd = jnp.dot(odd_left[...], basis[tile, 1], preferred_element_type=jnp.float32)
        for half, value in enumerate((even + odd, even - odd)):
            to = half * HALF + at
            staged[:, :, to : to + TILE] = value.astype(jnp.bfloat16).reshape(rows, fields, TILE)
            copy(half, tile).start()
    for tile in range(HALF // TILE):
        for half in range(2):
            copy(half, tile).wait()


def wave_of(received, basis, pairs, blocks, rows, fields):
    depth = 2 * pairs * blocks
    vmem = pl.BlockSpec(memory_space=pltpu.VMEM)
    return pl.pallas_call(
        functools.partial(wave_body, pairs=pairs, blocks=blocks, rows=rows, fields=fields),
        in_specs=[vmem, pl.BlockSpec(memory_space=pltpu.HBM)],
        out_specs=[pl.BlockSpec(memory_space=pltpu.HBM), vmem],
        out_shape=[
            jax.ShapeDtypeStruct((rows, fields, NLON), jnp.bfloat16),
            jax.ShapeDtypeStruct((1, fields), jnp.float32),
        ],
        scratch_shapes=[
            pltpu.VMEM((received.size // (2 * fields), 2 * fields), jnp.float32),
            pltpu.VMEM((rows * fields, depth), jnp.bfloat16),
            pltpu.VMEM((rows * fields, depth), jnp.bfloat16),
            pltpu.VMEM((HALF // TILE, 2, depth, TILE), jnp.bfloat16),
            pltpu.VMEM((rows, fields, NLON), jnp.bfloat16),
            pltpu.SemaphoreType.DMA((3, HALF // TILE)),
        ],
        compiler_params=pltpu.CompilerParams(vmem_limit_bytes=60 * 2**20),
        name="wave",
    )(received, basis)


def shards(load_coef, legendre, slab_orders, cycle_rows):
    blocks = lax.axis_size(BLK)
    pairs, slab_rows, fields2 = load_coef.shape
    lat = legendre.shape[2]
    rows = lat // blocks
    spectra = spectra_of(load_coef, legendre, slab_orders, cycle_rows, blocks)
    received = lax.all_to_all(spectra, BLK, split_axis=0, concat_axis=0, tiled=True)
    basis = basis_of(slab_orders, pairs, blocks, slab_rows - 2)
    wave, energy = wave_of(received, basis, pairs, blocks, rows, fields2 // 2)
    return wave, energy.reshape(fields2 // 2)


def solution(mesh):
    split = Mesh(
        mesh.devices.reshape(4, 4, 4, 2, mesh.shape["rep"]),
        ("blk_0", "blk_1", "blk_2", "blk_3", "rep"),
    )
    in_specs = (P(BLK, None, "rep"), P(BLK, None, None), P(), P())
    out_specs = (P(BLK, "rep", None), P("rep"))
    return jax.shard_map(
        shards, mesh=split, in_specs=in_specs, out_specs=out_specs, check_vma=False
    )
```

```python
import functools
import math

import jax
import jax.numpy as jnp
from jax import lax
from jax.experimental import pallas as pl
from jax.experimental.pallas import tpu as pltpu
from jax.sharding import Mesh
from jax.sharding import PartitionSpec as P


NLON = 4096
HALF = NLON // 2
BLK = ("blk_0", "blk_1", "blk_2", "blk_3")
DEPTH = 512
TILE = 256


def spectra_body(orders, cycles, coef_hbm, table_hbm, out, coef, table, tail, low_sum, high_sum, moved_out, energy_out, sems, *, slab_rows, depth):
    pairs, fields2 = coef_hbm.shape[1], coef_hbm.shape[2]
    lat = table_hbm.shape[2]
    chunks = slab_rows // depth
    whole = chunks * depth
    columns = lat // 128

    table_rows = table_hbm.reshape(slab_rows * pairs, lat)

    def piece(chunk, column):
        return pltpu.make_async_copy(
            table_rows.at[pl.ds(chunk * depth * pairs, depth * pairs), pl.ds(column * 128, 128)],
            table.at[chunk, column],
            sems.at[chunk, column],
        )

    def last(column):
        return pltpu.make_async_copy(
            table_hbm.at[pl.ds(whole, 1), :, pl.ds(column * 128, 128)],
            tail.at[column, pl.ds(0, 1)],
            sems.at[chunks, column],
        )

    coef_copy = pltpu.make_async_copy(
        coef_hbm.reshape(slab_rows * pairs, fields2), coef.at[pl.ds(0, slab_rows * pairs)], sems.at[chunks + 1, 0]
    )
    coef_copy.start()
    for column in range(columns):
        piece(0, column).start()
    for column in range(columns):
        last(column).start()
    for chunk in range(1, chunks):
        for column in range(columns):
            piece(chunk, column).start()

    first = lax.axis_index(BLK) * pairs
    lows = [orders[first + pair] for pair in range(pairs)]
    coef_copy.wait()

    def left_of(start, count, side):
        turned = coef[start * pairs : (start + count) * pairs, :].astype(jnp.float32).T
        lane = lax.broadcasted_iota(jnp.int32, turned.shape, 1)
        parts = []
        for pair in range(pairs):
            mine = lane % pairs == pair
            row = start + lane // pairs
            if side == "low":
                mine = mine & (row < slab_rows - 1 - lows[pair])
            elif side == "high":
                mine = mine & (row >= slab_rows - 1 - lows[pair]) & (row < slab_rows)
            parts.append(jnp.where(mine, turned, 0.0))
        return jnp.concatenate(parts, axis=0).astype(jnp.bfloat16)

    for column in range(columns):
        last(column).wait()
    ends = []
    for column in range(columns):
        end = tail.at[column].reshape(tail.shape[1] * pairs, 128)[...].astype(jnp.float32)
        keep = lax.broadcasted_iota(jnp.int32, end.shape, 0) < pairs
        ends.append(jnp.where(keep, end, 0.0).astype(jnp.bfloat16))
    ends = jnp.concatenate(ends, axis=1)
    high_sum[...] = jnp.dot(left_of(whole, tail.shape[1], "high"), ends, preferred_element_type=jnp.float32)

    for chunk in range(chunks):
        start = chunk * depth
        sure = start + depth <= slab_rows // 2
        low_left = left_of(start, depth, None if sure else "low")
        high_left = None if sure else left_of(start, depth, "high")
        for column in range(columns):
            piece(chunk, column).wait()
        right = jnp.concatenate(
            [table[chunk, column] for column in range(columns)], axis=1
        )
        low = jnp.dot(low_left, right, preferred_element_type=jnp.float32)
        low_sum[...] = low if chunk == 0 else low_sum[...] + low
        if not sure:
            high_sum[...] += jnp.dot(high_left, right, preferred_element_type=jnp.float32)

    spectrum = []
    for pair in range(pairs):
        even = lows[pair] % 2 == 0
        low = low_sum[pair * fields2 : (pair + 1) * fields2, :]
        high = high_sum[pair * fields2 : (pair + 1) * fields2, :]
        spectrum.append(jnp.where(even, low, high).astype(jnp.bfloat16))
        spectrum.append(jnp.where(even, high, low).astype(jnp.bfloat16))
    spectrum = jnp.concatenate(spectrum, axis=0)

    lane = lax.broadcasted_iota(jnp.int32, (128, lat), 1)
    onehot = []
    for at in range(0, lat, 128):
        column = jnp.broadcast_to(cycles[:, at : at + 128], (128, 128)).T
        column = jnp.concatenate([column] * columns, axis=1)
        onehot.append((column == lane).astype(jnp.float32).astype(jnp.bfloat16))
    onehot = jnp.concatenate(onehot, axis=0)
    moved = lax.dot_general(onehot, spectrum, (((1,), (1,)), ((), ())), preferred_element_type=jnp.float32)
    groups, blocks, rows, _ = moved_out.shape
    slabs = out.reshape(blocks, groups * rows + 2, fields2)
    copies = []
    for group in range(groups):
        part = moved[:, group * fields2 : (group + 1) * fields2].astype(jnp.bfloat16)
        moved_out[group] = part.reshape(blocks, rows, fields2)
        copies.append(
            pltpu.make_async_copy(
                moved_out.at[group], slabs.at[:, pl.ds(group * rows, rows)], sems.at[chunks + 1, 1 + group]
            )
        )
        copies[-1].start()

    sums = jnp.sum(moved * moved, axis=0, keepdims=True)
    lane = lax.broadcasted_iota(jnp.int32, (1, fields2), 1)
    real = lane < fields2 // 2
    total = jnp.zeros((1, fields2), jnp.float32)
    for pair in range(pairs):
        weight = jnp.where(lows[pair] == 0, jnp.where(real, 1.0, 0.0), 2.0)
        at = 2 * pair * fields2
        total = total + sums[:, at : at + fields2] * weight + sums[:, at + fields2 : at + 2 * fields2] * 2.0
    total = (total + pltpu.roll(total, fields2 // 2, 1)) * (1.0 / lat)
    top = total.astype(jnp.bfloat16).astype(jnp.float32)
    middle = (total - top).astype(jnp.bfloat16).astype(jnp.float32)
    bottom = total - top - middle
    first_row = jnp.where(real, top, middle)
    second_row = jnp.where(real, bottom, 0.0)
    tile = jnp.concatenate([first_row, second_row], axis=0).astype(jnp.bfloat16)
    energy_out[...] = jnp.broadcast_to(tile[None], energy_out.shape)
    copies.append(
        pltpu.make_async_copy(energy_out, out.at[:, groups * rows // 2], sems.at[chunks + 1, 1 + groups])
    )
    copies[-1].start()
    for copy in copies:
        copy.wait()


def spectra_of(load_coef, legendre, slab_orders, cycle_rows, blocks):
    pairs, slab_rows, fields2 = load_coef.shape
    lat = legendre.shape[2]
    columns = lat // 128
    chunks = slab_rows // DEPTH
    tiles = lat // blocks // 2
    anywhere = pl.BlockSpec(memory_space=pltpu.HBM)
    vmem = pl.BlockSpec(memory_space=pltpu.VMEM)
    return pl.pallas_call(
        functools.partial(spectra_body, slab_rows=slab_rows, depth=DEPTH),
        in_specs=[pl.BlockSpec(memory_space=pltpu.SMEM), vmem, anywhere, anywhere],
        out_specs=anywhere,
        out_shape=jax.ShapeDtypeStruct((blocks, pairs * 2 * tiles + 1, 2, fields2), jnp.bfloat16),
        scratch_shapes=[
            pltpu.VMEM(((slab_rows // 64 * 64 + 64) * pairs, fields2), jnp.bfloat16),
            pltpu.VMEM((chunks, columns, DEPTH * pairs, 128), jnp.bfloat16),
            pltpu.VMEM((columns, 8, pairs, 128), jnp.bfloat16),
            pltpu.VMEM((pairs * fields2, lat), jnp.float32),
            pltpu.VMEM((pairs * fields2, lat), jnp.float32),
            pltpu.VMEM((pairs * 2, blocks, tiles * 2, fields2), jnp.bfloat16),
            pltpu.VMEM((blocks, 2, fields2), jnp.bfloat16),
            pltpu.SemaphoreType.DMA((chunks + 2, columns)),
        ],
        compiler_params=pltpu.CompilerParams(vmem_limit_bytes=60 * 2**20),
        name="spectra",
    )(slab_orders, cycle_rows.reshape(1, lat), jnp.transpose(load_coef, (1, 0, 2)), jnp.transpose(legendre, (1, 0, 2)))


def angles_body(orders, out, columns, *, pairs, blocks, degree):
    count = pairs * blocks
    columns[...] = jnp.broadcast_to(orders[...], (128, count)).T
    lane = lax.broadcasted_iota(jnp.int32, (blocks, 128), 1)
    scale = 2.0 * math.pi / NLON
    for pair in range(pairs):
        low = columns[pl.ds(pair, blocks, stride=pairs), :]
        high = degree - low
        is_even = low % 2 == 0
        for parity, order in enumerate((jnp.where(is_even, low, high), jnp.where(is_even, high, low))):
            fine = (order * lane % NLON).astype(jnp.float32) * scale
            turn = (order * 128 % NLON).astype(jnp.float32) * scale
            factor = jnp.where(order == 0, 1.0, 2.0)
            at = pl.ds(pair * blocks, blocks)
            out[parity, 0, at, :] = factor * jnp.cos(fine)
            out[parity, 1, at, :] = -factor * jnp.sin(fine)
            out[parity, 2, at, :] = jnp.cos(turn)
            out[parity, 3, at, :] = jnp.sin(turn)


def angles_of(slab_orders, pairs, blocks, degree):
    return pl.pallas_call(
        functools.partial(angles_body, pairs=pairs, blocks=blocks, degree=degree),
        in_specs=[pl.BlockSpec(memory_space=pltpu.VMEM)],
        out_specs=pl.BlockSpec(memory_space=pltpu.VMEM),
        out_shape=jax.ShapeDtypeStruct((2, 4, pairs * blocks, 128), jnp.float32),
        scratch_shapes=[pltpu.VMEM((pairs * blocks, 128), jnp.int32)],
        compiler_params=pltpu.CompilerParams(vmem_limit_bytes=12 * 2**20),
        name="angles",
    )(slab_orders.reshape(1, pairs * blocks))


def wave_body(received, angles_in, out, energy, slabs, wide, angles, lefts, basis, staged, sems, *, pairs, blocks, rows, fields):
    tiles = HALF // TILE
    stride = slabs.shape[0] // blocks
    angles_copy = pltpu.make_async_copy(angles_in, angles, sems.at[2, 0])
    angles_copy.start()
    slabs_copy = pltpu.make_async_copy(received.reshape(*slabs.shape), slabs, sems.at[2, 1])
    slabs_copy.start()

    def build(tile):
        for parity in range(2):
            for pair in range(pairs):
                at = pl.ds(pair * blocks, blocks)
                cosine, sine = angles[parity, 0, at, :], angles[parity, 1, at, :]
                turn_cos, turn_sin = angles[parity, 2, at, :], angles[parity, 3, at, :]
                for lane in range(0, TILE, 128):
                    to = slice(lane, lane + 128)
                    basis[tile, parity, pl.ds(2 * pair * blocks, blocks), to] = cosine.astype(jnp.bfloat16)
                    basis[tile, parity, pl.ds((2 * pair + 1) * blocks, blocks), to] = sine.astype(jnp.bfloat16)
                    cosine, sine = cosine * turn_cos + sine * turn_sin, sine * turn_cos - cosine * turn_sin
                angles[parity, 0, at, :] = cosine
                angles[parity, 1, at, :] = sine

    angles_copy.wait()
    build(0)
    slabs_copy.wait()
    wide[...] = slabs[...].astype(jnp.float32)
    for pair in range(pairs):
        for parity in range(2):
            for row in range(rows):
                at = (pair * 2 + parity) * rows + row
                turned = wide[pl.ds(at, blocks, stride=stride), :].T.astype(jnp.bfloat16)
                for part in range(2):
                    to = (pair * 2 + part) * blocks
                    lefts[parity, row * fields : (row + 1) * fields, to : to + blocks] = turned[
                        part * fields : (part + 1) * fields, :
                    ]

    def copy(half, tile):
        at = half * HALF + tile * TILE
        return pltpu.make_async_copy(
            staged.at[:, :, pl.ds(at, TILE)], out.at[:, :, pl.ds(at, TILE)], sems.at[half, tile]
        )

    for tile in range(tiles):
        at = tile * TILE
        even = jnp.dot(lefts[0], basis[tile, 0], preferred_element_type=jnp.float32)
        odd = jnp.dot(lefts[1], basis[tile, 1], preferred_element_type=jnp.float32)
        if tile + 1 < tiles:
            build(tile + 1)
        for half, value in enumerate((even + odd, even - odd)):
            to = half * HALF + at
            staged[:, :, to : to + TILE] = value.astype(jnp.bfloat16).reshape(rows, fields, TILE)
            copy(half, tile).start()

    at = 2 * pairs * rows
    parts = wide[pl.ds(at, blocks, stride=stride), :] + wide[pl.ds(at + 1, blocks, stride=stride), :]
    total = jnp.sum(parts, axis=0, keepdims=True)
    energy[...] = (total + pltpu.roll(total, fields, 1))[:, :fields]
    for tile in range(tiles):
        for half in range(2):
            copy(half, tile).wait()


def wave_of(received, angles, pairs, blocks, rows, fields):
    depth = 2 * pairs * blocks
    tiles = HALF // TILE
    anywhere = pl.BlockSpec(memory_space=pl.ANY)
    flat = (received.size // (2 * fields), 2 * fields)
    return pl.pallas_call(
        functools.partial(wave_body, pairs=pairs, blocks=blocks, rows=rows, fields=fields),
        in_specs=[anywhere, anywhere],
        out_specs=[pl.BlockSpec(memory_space=pltpu.HBM), pl.BlockSpec(memory_space=pltpu.VMEM)],
        out_shape=[
            jax.ShapeDtypeStruct((rows, fields, NLON), jnp.bfloat16),
            jax.ShapeDtypeStruct((1, fields), jnp.float32),
        ],
        scratch_shapes=[
            pltpu.VMEM(flat, jnp.bfloat16),
            pltpu.VMEM(flat, jnp.float32),
            pltpu.VMEM(angles.shape, jnp.float32),
            pltpu.VMEM((2, rows * fields, depth), jnp.bfloat16),
            pltpu.VMEM((tiles, 2, depth, TILE), jnp.bfloat16),
            pltpu.VMEM((rows, fields, NLON), jnp.bfloat16),
            pltpu.SemaphoreType.DMA((3, tiles)),
        ],
        compiler_params=pltpu.CompilerParams(vmem_limit_bytes=24 * 2**20),
        name="wave",
    )(received, angles)


def shards(load_coef, legendre, slab_orders, cycle_rows):
    blocks = lax.axis_size(BLK)
    pairs, slab_rows, fields2 = load_coef.shape
    lat = legendre.shape[2]
    rows = lat // blocks
    spectra = spectra_of(load_coef, legendre, slab_orders, cycle_rows, blocks)
    received = lax.all_to_all(spectra, BLK, split_axis=0, concat_axis=0, tiled=True)
    angles = angles_of(slab_orders, pairs, blocks, slab_rows - 2)
    wave, energy = wave_of(received, angles, pairs, blocks, rows, fields2 // 2)
    return wave, energy.reshape(fields2 // 2)


def solution(mesh):
    split = Mesh(
        mesh.devices.reshape(4, 4, 4, 2, mesh.shape["rep"]),
        ("blk_0", "blk_1", "blk_2", "blk_3", "rep"),
    )
    in_specs = (P(BLK, None, "rep"), P(BLK, None, None), P(), P())
    out_specs = (P(BLK, "rep", None), P("rep"))
    return jax.shard_map(
        shards, mesh=split, in_specs=in_specs, out_specs=out_specs, check_vma=False
    )
```

```python
import functools
import math

import jax
import jax.numpy as jnp
from jax import lax
from jax.experimental import pallas as pl
from jax.experimental.pallas import tpu as pltpu
from jax.sharding import Mesh
from jax.sharding import PartitionSpec as P


NLON = 4096
HALF = NLON // 2
BLK = ("blk_0", "blk_1", "blk_2", "blk_3")
WIDTH = 256
PART = 256
TILE = 256


def spectra_body(
    orders, cycles, coef_hbm, table_hbm, out, coef, table, tail, low_left, high_left, onehot, moved, parts_out, energy_out, sems, *, slab_rows
):
    pairs, fields2 = coef_hbm.shape[1], coef_hbm.shape[2]
    lat = table_hbm.shape[2]
    columns = lat // 128
    packed = slab_rows * pairs
    depth = table.shape[1]
    middle = depth - (high_left.shape[1] - 128)

    coef_copy = pltpu.make_async_copy(coef_hbm.reshape(packed, fields2), coef.at[pl.ds(0, packed)], sems.at[2, 0])
    coef_copy.start()
    table_rows = table_hbm.reshape(packed, lat)
    pieces = []
    for column in range(columns):
        lanes = pl.ds(column * 128, 128)
        piece = pltpu.make_async_copy(table_rows.at[pl.ds(0, depth), lanes], table.at[column], sems.at[0, column])
        last = pltpu.make_async_copy(
            table_hbm.at[pl.ds(slab_rows - 1, 1), :, lanes], tail.at[column, pl.ds(0, 1)], sems.at[1, column]
        )
        piece.start()
        last.start()
        pieces.append((piece, last))

    lane = lax.broadcasted_iota(jnp.int32, (128, lat), 1)
    for at in range(0, lat, 128):
        column = jnp.broadcast_to(cycles[:, at : at + 128], (128, 128)).T
        column = jnp.concatenate([column] * columns, axis=1)
        onehot[at : at + 128, :] = (column == lane).astype(jnp.float32).astype(jnp.bfloat16)

    first = lax.axis_index(BLK) * pairs
    lows = [orders[first + pair] for pair in range(pairs)]
    coef_copy.wait()
    for at in range(0, depth + 128, 128):
        turned = coef[at : at + 128, :].astype(jnp.float32).T
        place = at + lax.broadcasted_iota(jnp.int32, turned.shape, 1)
        row = place // pairs
        for pair in range(pairs):
            mine = place % pairs == pair
            to = slice(pair * fields2, (pair + 1) * fields2)
            in_low = row < slab_rows - 1 - lows[pair]
            if at < middle:
                low_left[to, at : at + 128] = jnp.where(mine, turned, 0.0).astype(jnp.bfloat16)
                continue
            if at < depth:
                low_left[to, at : at + 128] = jnp.where(mine & in_low, turned, 0.0).astype(jnp.bfloat16)
            in_high = mine & ~in_low & (row < slab_rows)
            high_left[to, at - middle : at - middle + 128] = jnp.where(in_high, turned, 0.0).astype(jnp.bfloat16)

    groups, blocks, rows, _ = parts_out.shape
    slabs = out.reshape(blocks, groups * rows + 2, fields2)
    copies = []
    sums = jnp.zeros((1, groups * fields2), jnp.float32)
    for at in range(0, lat, WIDTH):
        tiles = range(at // 128, (at + WIDTH) // 128)
        for column in tiles:
            for copy in pieces[column]:
                copy.wait()
        right = jnp.concatenate([table[column] for column in tiles], axis=1)
        low_all = jnp.dot(low_left[...], right, preferred_element_type=jnp.float32)
        right = jnp.concatenate([table[column, middle:, :] for column in tiles], axis=1)
        high_all = jnp.dot(high_left[:, : depth - middle], right, preferred_element_type=jnp.float32)
        ends = []
        for column in tiles:
            end = tail.at[column].reshape(tail.shape[1] * pairs, 128)[...].astype(jnp.float32)
            keep = lax.broadcasted_iota(jnp.int32, end.shape, 0) < pairs
            ends.append(jnp.where(keep, end, 0.0).astype(jnp.bfloat16))
        ends = jnp.concatenate(ends, axis=1)
        end_left = high_left[:, depth - middle : depth - middle + ends.shape[0]]
        high_all = high_all + jnp.dot(end_left, ends, preferred_element_type=jnp.float32)
        spectrum = []
        for pair in range(pairs):
            even = lows[pair] % 2 == 0
            low = low_all[pair * fields2 : (pair + 1) * fields2, :]
            high = high_all[pair * fields2 : (pair + 1) * fields2, :]
            spectrum.append(jnp.where(even, low, high).astype(jnp.bfloat16))
            spectrum.append(jnp.where(even, high, low).astype(jnp.bfloat16))
        spectrum = jnp.concatenate(spectrum, axis=0)
        for start in range(0, lat, PART):
            share = lax.dot_general(
                onehot[start : start + PART, at : at + WIDTH],
                spectrum,
                (((1,), (1,)), ((), ())),
                preferred_element_type=jnp.float32,
            )
            if at > 0:
                share = moved[start : start + PART, :] + share
            if at + WIDTH < lat:
                moved[start : start + PART, :] = share
                continue
            sums = sums + jnp.sum(share * share, axis=0, keepdims=True)
            block = pl.ds(start // rows, PART // rows)
            for group in range(groups):
                part = share[:, group * fields2 : (group + 1) * fields2].astype(jnp.bfloat16)
                parts_out[group, block] = part.reshape(PART // rows, rows, fields2)
                copies.append(
                    pltpu.make_async_copy(
                        parts_out.at[group, block],
                        slabs.at[block, pl.ds(group * rows, rows)],
                        sems.at[3, len(copies)],
                    )
                )
                copies[-1].start()

    lane = lax.broadcasted_iota(jnp.int32, (1, fields2), 1)
    real = lane < fields2 // 2
    total = jnp.zeros((1, fields2), jnp.float32)
    for pair in range(pairs):
        weight = jnp.where(lows[pair] == 0, jnp.where(real, 1.0, 0.0), 2.0)
        at = 2 * pair * fields2
        total = total + sums[:, at : at + fields2] * weight + sums[:, at + fields2 : at + 2 * fields2] * 2.0
    total = (total + pltpu.roll(total, fields2 // 2, 1)) * (1.0 / lat)
    top = total.astype(jnp.bfloat16).astype(jnp.float32)
    next_bits = (total - top).astype(jnp.bfloat16).astype(jnp.float32)
    bottom = total - top - next_bits
    first_row = jnp.where(real, top, next_bits)
    second_row = jnp.where(real, bottom, 0.0)
    tile = jnp.concatenate([first_row, second_row], axis=0).astype(jnp.bfloat16)
    energy_out[...] = jnp.broadcast_to(tile[None], energy_out.shape)
    copies.append(
        pltpu.make_async_copy(energy_out, out.at[:, groups * rows // 2], sems.at[3, len(copies)])
    )
    copies[-1].start()
    for copy in copies:
        copy.wait()


def spectra_of(load_coef, legendre, slab_orders, cycle_rows, blocks):
    pairs, slab_rows, fields2 = load_coef.shape
    lat = legendre.shape[2]
    columns = lat // 128
    rows = lat // blocks
    lower = (slab_rows - 1) * pairs
    middle = (slab_rows - 1) // 2 * pairs
    anywhere = pl.BlockSpec(memory_space=pltpu.HBM)
    vmem = pl.BlockSpec(memory_space=pltpu.VMEM)
    return pl.pallas_call(
        functools.partial(spectra_body, slab_rows=slab_rows),
        in_specs=[pl.BlockSpec(memory_space=pltpu.SMEM), vmem, anywhere, anywhere],
        out_specs=anywhere,
        out_shape=jax.ShapeDtypeStruct((blocks, pairs * rows + 1, 2, fields2), jnp.bfloat16),
        scratch_shapes=[
            pltpu.VMEM((lower + 128, fields2), jnp.bfloat16),
            pltpu.VMEM((columns, lower, 128), jnp.bfloat16),
            pltpu.VMEM((columns, 8, pairs, 128), jnp.bfloat16),
            pltpu.VMEM((pairs * fields2, lower), jnp.bfloat16),
            pltpu.VMEM((pairs * fields2, lower + 128 - middle), jnp.bfloat16),
            pltpu.VMEM((lat, lat), jnp.bfloat16),
            pltpu.VMEM((lat, 2 * pairs * fields2), jnp.float32),
            pltpu.VMEM((2 * pairs, blocks, rows, fields2), jnp.bfloat16),
            pltpu.VMEM((blocks, 2, fields2), jnp.bfloat16),
            pltpu.SemaphoreType.DMA((4, max(columns, 2 * pairs * (lat // PART) + 1))),
        ],
        compiler_params=pltpu.CompilerParams(vmem_limit_bytes=60 * 2**20),
        name="spectra",
    )(slab_orders, cycle_rows.reshape(1, lat), jnp.transpose(load_coef, (1, 0, 2)), jnp.transpose(legendre, (1, 0, 2)))


def angles_body(orders, out, columns, *, pairs, blocks, degree):
    count = pairs * blocks
    columns[...] = jnp.broadcast_to(orders[...], (128, count)).T
    lane = lax.broadcasted_iota(jnp.int32, (blocks, 128), 1)
    scale = 2.0 * math.pi / NLON
    for pair in range(pairs):
        low = columns[pl.ds(pair, blocks, stride=pairs), :]
        high = degree - low
        is_even = low % 2 == 0
        for parity, order in enumerate((jnp.where(is_even, low, high), jnp.where(is_even, high, low))):
            fine = (order * lane % NLON).astype(jnp.float32) * scale
            turn = (order * 128 % NLON).astype(jnp.float32) * scale
            factor = jnp.where(order == 0, 1.0, 2.0)
            at = pl.ds(pair * blocks, blocks)
            out[parity, 0, at, :] = factor * jnp.cos(fine)
            out[parity, 1, at, :] = -factor * jnp.sin(fine)
            out[parity, 2, at, :] = jnp.cos(turn)
            out[parity, 3, at, :] = jnp.sin(turn)


def angles_of(slab_orders, pairs, blocks, degree):
    return pl.pallas_call(
        functools.partial(angles_body, pairs=pairs, blocks=blocks, degree=degree),
        in_specs=[pl.BlockSpec(memory_space=pltpu.VMEM)],
        out_specs=pl.BlockSpec(memory_space=pltpu.VMEM),
        out_shape=jax.ShapeDtypeStruct((2, 4, pairs * blocks, 128), jnp.float32),
        scratch_shapes=[pltpu.VMEM((pairs * blocks, 128), jnp.int32)],
        compiler_params=pltpu.CompilerParams(vmem_limit_bytes=12 * 2**20),
        name="angles",
    )(slab_orders.reshape(1, pairs * blocks))


def wave_body(received, angles, out, energy, slabs, wide, state, lefts, basis, staged, sems, *, pairs, blocks, rows, fields):
    tiles = HALF // TILE
    stride = slabs.shape[0] // blocks
    slabs_copy = pltpu.make_async_copy(received.reshape(*slabs.shape), slabs, sems.at[2, 1])
    slabs_copy.start()

    def build(tile):
        for parity in range(2):
            for pair in range(pairs):
                at = pl.ds(pair * blocks, blocks)
                held = angles if tile == 0 else state
                cosine, sine = held[parity, 0, at, :], held[parity, 1, at, :]
                turn_cos, turn_sin = angles[parity, 2, at, :], angles[parity, 3, at, :]
                for lane in range(0, TILE, 128):
                    to = slice(lane, lane + 128)
                    basis[tile, parity, pl.ds(2 * pair * blocks, blocks), to] = cosine.astype(jnp.bfloat16)
                    basis[tile, parity, pl.ds((2 * pair + 1) * blocks, blocks), to] = sine.astype(jnp.bfloat16)
                    cosine, sine = cosine * turn_cos + sine * turn_sin, sine * turn_cos - cosine * turn_sin
                state[parity, 0, at, :] = cosine
                state[parity, 1, at, :] = sine

    build(0)
    slabs_copy.wait()
    wide[...] = slabs[...].astype(jnp.float32)
    for pair in range(pairs):
        for parity in range(2):
            for row in range(rows):
                at = (pair * 2 + parity) * rows + row
                turned = wide[pl.ds(at, blocks, stride=stride), :].T.astype(jnp.bfloat16)
                for part in range(2):
                    to = (pair * 2 + part) * blocks
                    lefts[parity, row * fields : (row + 1) * fields, to : to + blocks] = turned[
                        part * fields : (part + 1) * fields, :
                    ]

    def copy(half, tile):
        at = half * HALF + tile * TILE
        return pltpu.make_async_copy(
            staged.at[:, :, pl.ds(at, TILE)], out.at[:, :, pl.ds(at, TILE)], sems.at[half, tile]
        )

    for tile in range(tiles):
        at = tile * TILE
        even = jnp.dot(lefts[0], basis[tile, 0], preferred_element_type=jnp.float32)
        odd = jnp.dot(lefts[1], basis[tile, 1], preferred_element_type=jnp.float32)
        if tile + 1 < tiles:
            build(tile + 1)
        for half, value in enumerate((even + odd, even - odd)):
            to = half * HALF + at
            staged[:, :, to : to + TILE] = value.astype(jnp.bfloat16).reshape(rows, fields, TILE)
            copy(half, tile).start()

    at = 2 * pairs * rows
    parts = wide[pl.ds(at, blocks, stride=stride), :] + wide[pl.ds(at + 1, blocks, stride=stride), :]
    total = jnp.sum(parts, axis=0, keepdims=True)
    energy[...] = (total + pltpu.roll(total, fields, 1))[:, :fields]
    for tile in range(tiles):
        for half in range(2):
            copy(half, tile).wait()


def wave_of(received, angles, pairs, blocks, rows, fields):
    depth = 2 * pairs * blocks
    tiles = HALF // TILE
    anywhere = pl.BlockSpec(memory_space=pl.ANY)
    flat = (received.size // (2 * fields), 2 * fields)
    return pl.pallas_call(
        functools.partial(wave_body, pairs=pairs, blocks=blocks, rows=rows, fields=fields),
        in_specs=[anywhere, pl.BlockSpec(memory_space=pltpu.VMEM)],
        out_specs=[pl.BlockSpec(memory_space=pltpu.HBM), pl.BlockSpec(memory_space=pltpu.VMEM)],
        out_shape=[
            jax.ShapeDtypeStruct((rows, fields, NLON), jnp.bfloat16),
            jax.ShapeDtypeStruct((1, fields), jnp.float32),
        ],
        scratch_shapes=[
            pltpu.VMEM(flat, jnp.bfloat16),
            pltpu.VMEM(flat, jnp.float32),
            pltpu.VMEM((2, 2, *angles.shape[2:]), jnp.float32),
            pltpu.VMEM((2, rows * fields, depth), jnp.bfloat16),
            pltpu.VMEM((tiles, 2, depth, TILE), jnp.bfloat16),
            pltpu.VMEM((rows, fields, NLON), jnp.bfloat16),
            pltpu.SemaphoreType.DMA((3, tiles)),
        ],
        compiler_params=pltpu.CompilerParams(vmem_limit_bytes=24 * 2**20),
        name="wave",
    )(received, angles)


def shards(load_coef, legendre, slab_orders, cycle_rows):
    blocks = lax.axis_size(BLK)
    pairs, slab_rows, fields2 = load_coef.shape
    lat = legendre.shape[2]
    rows = lat // blocks
    spectra = spectra_of(load_coef, legendre, slab_orders, cycle_rows, blocks)
    received = lax.all_to_all(spectra, BLK, split_axis=0, concat_axis=0, tiled=True)
    angles = angles_of(slab_orders, pairs, blocks, slab_rows - 2)
    wave, energy = wave_of(received, angles, pairs, blocks, rows, fields2 // 2)
    return wave, energy.reshape(fields2 // 2)


def solution(mesh):
    split = Mesh(
        mesh.devices.reshape(4, 4, 4, 2, mesh.shape["rep"]),
        ("blk_0", "blk_1", "blk_2", "blk_3", "rep"),
    )
    in_specs = (P(BLK, None, "rep"), P(BLK, None, None), P(), P())
    out_specs = (P(BLK, "rep", None), P("rep"))
    return jax.shard_map(
        shards, mesh=split, in_specs=in_specs, out_specs=out_specs, check_vma=False
    )
```

```python
import functools
import math

import jax
import jax.numpy as jnp
from jax import lax
from jax.experimental import pallas as pl
from jax.experimental.pallas import tpu as pltpu
from jax.sharding import Mesh
from jax.sharding import PartitionSpec as P


NLON = 4096
HALF = NLON // 2
BLK = ("blk_0", "blk_1", "blk_2", "blk_3")
DEPTH = 512
TILE = 256
ORDER = (("blk_3", 2), ("blk_2", 4), ("blk_1", 4), ("blk_0", 4))


def spectra_body(orders_hbm, cycles_hbm, coef_hbm, table_hbm, out, energy_hbm, coef, table, tail, low_sum, high_sum, moved_out, energy, orders, cycles, sems, *, slab_rows, depth):
    pairs, fields2 = coef_hbm.shape[1], coef_hbm.shape[2]
    lat = table_hbm.shape[2]
    chunks = slab_rows // depth
    whole = chunks * depth
    columns = lat // 128

    table_rows = table_hbm.reshape(slab_rows * pairs, lat)

    def piece(chunk, column):
        return pltpu.make_async_copy(
            table_rows.at[pl.ds(chunk * depth * pairs, depth * pairs), pl.ds(column * 128, 128)],
            table.at[chunk, column],
            sems.at[chunk, column],
        )

    def last(column):
        return pltpu.make_async_copy(
            table_hbm.at[pl.ds(whole, 1), :, pl.ds(column * 128, 128)],
            tail.at[column, pl.ds(0, 1)],
            sems.at[chunks, column],
        )

    coef_copy = pltpu.make_async_copy(
        coef_hbm.reshape(slab_rows * pairs, fields2), coef.at[pl.ds(0, slab_rows * pairs)], sems.at[chunks + 1, 0]
    )
    coef_copy.start()
    orders_copy = pltpu.make_async_copy(orders_hbm, orders, sems.at[chunks + 2, 0])
    orders_copy.start()
    cycles_copy = pltpu.make_async_copy(cycles_hbm, cycles, sems.at[chunks + 2, 1])
    cycles_copy.start()
    for column in range(columns):
        piece(0, column).start()
    for column in range(columns):
        last(column).start()
    for chunk in range(1, chunks):
        for column in range(columns):
            piece(chunk, column).start()

    orders_copy.wait()
    cycles_copy.wait()
    first = lax.axis_index(BLK) * pairs
    lows = [orders[first + pair] for pair in range(pairs)]
    coef_copy.wait()

    def left_of(start, count, side):
        turned = coef[start * pairs : (start + count) * pairs, :].astype(jnp.float32).T
        lane = lax.broadcasted_iota(jnp.int32, turned.shape, 1)
        parts = []
        for pair in range(pairs):
            mine = lane % pairs == pair
            row = start + lane // pairs
            if side == "low":
                mine = mine & (row < slab_rows - 1 - lows[pair])
            elif side == "high":
                mine = mine & (row >= slab_rows - 1 - lows[pair]) & (row < slab_rows)
            parts.append(jnp.where(mine, turned, 0.0))
        return jnp.concatenate(parts, axis=0).astype(jnp.bfloat16)

    for column in range(columns):
        last(column).wait()
    ends = []
    for column in range(columns):
        end = tail.at[column].reshape(tail.shape[1] * pairs, 128)[...].astype(jnp.float32)
        keep = lax.broadcasted_iota(jnp.int32, end.shape, 0) < pairs
        ends.append(jnp.where(keep, end, 0.0).astype(jnp.bfloat16))
    ends = jnp.concatenate(ends, axis=1)
    high_sum[...] = jnp.dot(left_of(whole, tail.shape[1], "high"), ends, preferred_element_type=jnp.float32)

    for chunk in range(chunks):
        start = chunk * depth
        sure = start + depth <= slab_rows // 2
        low_left = left_of(start, depth, None if sure else "low")
        high_left = None if sure else left_of(start, depth, "high")
        for column in range(columns):
            piece(chunk, column).wait()
        right = jnp.concatenate(
            [table[chunk, column] for column in range(columns)], axis=1
        )
        low = jnp.dot(low_left, right, preferred_element_type=jnp.float32)
        low_sum[...] = low if chunk == 0 else low_sum[...] + low
        if not sure:
            high_sum[...] += jnp.dot(high_left, right, preferred_element_type=jnp.float32)

    spectrum = []
    for pair in range(pairs):
        even = lows[pair] % 2 == 0
        low = low_sum[pair * fields2 : (pair + 1) * fields2, :]
        high = high_sum[pair * fields2 : (pair + 1) * fields2, :]
        spectrum.append(jnp.where(even, low, high).astype(jnp.bfloat16))
        spectrum.append(jnp.where(even, high, low).astype(jnp.bfloat16))
    spectrum = jnp.concatenate(spectrum, axis=0)

    lane = lax.broadcasted_iota(jnp.int32, (128, lat), 1)
    onehot = []
    for at in range(0, lat, 128):
        column = jnp.broadcast_to(cycles[:, at : at + 128], (128, 128)).T
        column = jnp.concatenate([column] * columns, axis=1)
        onehot.append((column == lane).astype(jnp.float32).astype(jnp.bfloat16))
    onehot = jnp.concatenate(onehot, axis=0)
    moved = lax.dot_general(onehot, spectrum, (((1,), (1,)), ((), ())), preferred_element_type=jnp.float32)
    groups, blocks, rows, _ = moved_out.shape
    slabs = out.reshape(blocks, groups * rows, fields2)
    copies = []
    for group in range(groups):
        part = moved[:, group * fields2 : (group + 1) * fields2].astype(jnp.bfloat16)
        moved_out[group] = part.reshape(blocks, rows, fields2)
        copies.append(
            pltpu.make_async_copy(
                moved_out.at[group], slabs.at[:, pl.ds(group * rows, rows)], sems.at[chunks + 1, 1 + group]
            )
        )
        copies[-1].start()

    sums = jnp.sum(moved * moved, axis=0, keepdims=True)
    lane = lax.broadcasted_iota(jnp.int32, (1, fields2), 1)
    real = lane < fields2 // 2
    total = jnp.zeros((1, fields2), jnp.float32)
    for pair in range(pairs):
        weight = jnp.where(lows[pair] == 0, jnp.where(real, 1.0, 0.0), 2.0)
        at = 2 * pair * fields2
        total = total + sums[:, at : at + fields2] * weight + sums[:, at + fields2 : at + 2 * fields2] * 2.0
    total = (total + pltpu.roll(total, fields2 // 2, 1)) * (1.0 / lat)
    energy[...] = total
    copies.append(pltpu.make_async_copy(energy, energy_hbm, sems.at[chunks + 2, 2]))
    copies[-1].start()
    for copy in copies:
        copy.wait()


def spectra_of(load_coef, legendre, slab_orders, cycle_rows, blocks):
    pairs, slab_rows, fields2 = load_coef.shape
    lat = legendre.shape[2]
    columns = lat // 128
    chunks = slab_rows // DEPTH
    tiles = lat // blocks // 2
    anywhere = pl.BlockSpec(memory_space=pltpu.HBM)
    return pl.pallas_call(
        functools.partial(spectra_body, slab_rows=slab_rows, depth=DEPTH),
        in_specs=[anywhere] * 4,
        out_specs=[anywhere, anywhere],
        out_shape=[
            jax.ShapeDtypeStruct((blocks, pairs * 2 * tiles, 2, fields2), jnp.bfloat16),
            jax.ShapeDtypeStruct((1, fields2), jnp.float32),
        ],
        scratch_shapes=[
            pltpu.VMEM(((slab_rows // 64 * 64 + 64) * pairs, fields2), jnp.bfloat16),
            pltpu.VMEM((chunks, columns, DEPTH * pairs, 128), jnp.bfloat16),
            pltpu.VMEM((columns, 8, pairs, 128), jnp.bfloat16),
            pltpu.VMEM((pairs * fields2, lat), jnp.float32),
            pltpu.VMEM((pairs * fields2, lat), jnp.float32),
            pltpu.VMEM((pairs * 2, blocks, tiles * 2, fields2), jnp.bfloat16),
            pltpu.VMEM((1, fields2), jnp.float32),
            pltpu.SMEM(slab_orders.shape, jnp.int32),
            pltpu.VMEM((1, lat), jnp.int32),
            pltpu.SemaphoreType.DMA((chunks + 3, columns)),
        ],
        compiler_params=pltpu.CompilerParams(vmem_limit_bytes=60 * 2**20),
        name="spectra",
    )(slab_orders, cycle_rows.reshape(1, lat), jnp.transpose(load_coef, (1, 0, 2)), jnp.transpose(legendre, (1, 0, 2)))


def angles_body(orders, out, columns, *, pairs, blocks, degree):
    count = pairs * blocks
    columns[...] = jnp.broadcast_to(orders[...], (128, count)).T
    lane = lax.broadcasted_iota(jnp.int32, (blocks, 128), 1)
    scale = 2.0 * math.pi / NLON
    for pair in range(pairs):
        low = columns[pl.ds(pair, blocks, stride=pairs), :]
        high = degree - low
        is_even = low % 2 == 0
        for parity, order in enumerate((jnp.where(is_even, low, high), jnp.where(is_even, high, low))):
            fine = (order * lane % NLON).astype(jnp.float32) * scale
            turn = (order * 128 % NLON).astype(jnp.float32) * scale
            factor = jnp.where(order == 0, 1.0, 2.0)
            at = pl.ds(pair * blocks, blocks)
            out[parity, 0, at, :] = factor * jnp.cos(fine)
            out[parity, 1, at, :] = -factor * jnp.sin(fine)
            out[parity, 2, at, :] = jnp.cos(turn)
            out[parity, 3, at, :] = jnp.sin(turn)


def angles_of(slab_orders, pairs, blocks, degree):
    return pl.pallas_call(
        functools.partial(angles_body, pairs=pairs, blocks=blocks, degree=degree),
        in_specs=[pl.BlockSpec(memory_space=pltpu.VMEM)],
        out_specs=pl.BlockSpec(memory_space=pltpu.VMEM),
        out_shape=jax.ShapeDtypeStruct((2, 4, pairs * blocks, 128), jnp.float32),
        scratch_shapes=[pltpu.VMEM((pairs * blocks, 128), jnp.int32)],
        compiler_params=pltpu.CompilerParams(vmem_limit_bytes=12 * 2**20),
        name="angles",
    )(slab_orders.reshape(1, pairs * blocks))


def wave_body(received, angles_in, out, slabs, wide, angles, lefts, basis, staged, sems, *, pairs, blocks, rows, fields):
    tiles = HALF // TILE
    stride = wide.shape[1]
    angles_copy = pltpu.make_async_copy(angles_in, angles, sems.at[2, 0])
    angles_copy.start()
    slabs_copy = pltpu.make_async_copy(received.reshape(*slabs.shape), slabs, sems.at[2, 1])
    slabs_copy.start()

    def build(tile):
        for parity in range(2):
            for pair in range(pairs):
                at = pl.ds(pair * blocks, blocks)
                cosine, sine = angles[parity, 0, at, :], angles[parity, 1, at, :]
                turn_cos, turn_sin = angles[parity, 2, at, :], angles[parity, 3, at, :]
                for lane in range(0, TILE, 128):
                    to = slice(lane, lane + 128)
                    basis[tile, parity, pl.ds(2 * pair * blocks, blocks), to] = cosine.astype(jnp.bfloat16)
                    basis[tile, parity, pl.ds((2 * pair + 1) * blocks, blocks), to] = sine.astype(jnp.bfloat16)
                    cosine, sine = cosine * turn_cos + sine * turn_sin, sine * turn_cos - cosine * turn_sin
                angles[parity, 0, at, :] = cosine
                angles[parity, 1, at, :] = sine

    angles_copy.wait()
    build(0)
    slabs_copy.wait()
    per_slab = slabs.shape[0] // blocks
    wide[:, :per_slab, :] = slabs[...].astype(jnp.float32).reshape(blocks, per_slab, slabs.shape[1])
    spaced = wide.reshape(blocks * stride, slabs.shape[1])
    for pair in range(pairs):
        for parity in range(2):
            for row in range(rows):
                at = (pair * 2 + parity) * rows + row
                turned = spaced[pl.ds(at, blocks, stride=stride), :].T.astype(jnp.bfloat16)
                for part in range(2):
                    to = (pair * 2 + part) * blocks
                    lefts[parity, row * fields : (row + 1) * fields, to : to + blocks] = turned[
                        part * fields : (part + 1) * fields, :
                    ]

    def copy(half, tile):
        at = half * HALF + tile * TILE
        return pltpu.make_async_copy(
            staged.at[:, :, pl.ds(at, TILE)], out.at[:, :, pl.ds(at, TILE)], sems.at[half, tile]
        )

    for tile in range(tiles):
        at = tile * TILE
        even = jnp.dot(lefts[0], basis[tile, 0], preferred_element_type=jnp.float32)
        odd = jnp.dot(lefts[1], basis[tile, 1], preferred_element_type=jnp.float32)
        if tile + 1 < tiles:
            build(tile + 1)
        for half, value in enumerate((even + odd, even - odd)):
            to = half * HALF + at
            staged[:, :, to : to + TILE] = value.astype(jnp.bfloat16).reshape(rows, fields, TILE)
            copy(half, tile).start()

    for tile in range(tiles):
        for half in range(2):
            copy(half, tile).wait()


def wave_of(received, angles, pairs, blocks, rows, fields):
    depth = 2 * pairs * blocks
    tiles = HALF // TILE
    anywhere = pl.BlockSpec(memory_space=pl.ANY)
    flat = (received.size // (2 * fields), 2 * fields)
    return pl.pallas_call(
        functools.partial(wave_body, pairs=pairs, blocks=blocks, rows=rows, fields=fields),
        in_specs=[anywhere, anywhere],
        out_specs=pl.BlockSpec(memory_space=pltpu.HBM),
        out_shape=jax.ShapeDtypeStruct((rows, fields, NLON), jnp.bfloat16),
        scratch_shapes=[
            pltpu.VMEM(flat, jnp.bfloat16),
            pltpu.VMEM((blocks, flat[0] // blocks + 8, flat[1]), jnp.float32),
            pltpu.VMEM(angles.shape, jnp.float32),
            pltpu.VMEM((2, rows * fields, depth), jnp.bfloat16),
            pltpu.VMEM((tiles, 2, depth, TILE), jnp.bfloat16),
            pltpu.VMEM((rows, fields, NLON), jnp.bfloat16),
            pltpu.SemaphoreType.DMA((3, tiles)),
        ],
        compiler_params=pltpu.CompilerParams(vmem_limit_bytes=24 * 2**20),
        name="wave",
    )(received, angles)


def shards(load_coef, legendre, slab_orders, cycle_rows):
    blocks = lax.axis_size(BLK)
    pairs, slab_rows, fields2 = load_coef.shape
    lat = legendre.shape[2]
    rows = lat // blocks
    spectra, energy = spectra_of(load_coef, legendre, slab_orders, cycle_rows, blocks)
    received = lax.all_to_all(spectra, BLK, split_axis=0, concat_axis=0, tiled=True)
    angles = angles_of(slab_orders, pairs, blocks, slab_rows - 2)
    for axis, size in ORDER:
        other = [
            lax.ppermute(energy, axis, [(at, at ^ step) for at in range(size)]) for step in range(1, size)
        ]
        energy = energy + other[0]
        if size == 4:
            energy = energy + (other[1] + other[2])
    wave = wave_of(received, angles, pairs, blocks, rows, fields2 // 2)
    return wave, energy[0, : fields2 // 2]


def solution(mesh):
    split = Mesh(
        mesh.devices.reshape(4, 4, 4, 2, mesh.shape["rep"]),
        ("blk_0", "blk_1", "blk_2", "blk_3", "rep"),
    )
    in_specs = (P(BLK, None, "rep"), P(BLK, None, None), P(), P())
    out_specs = (P(BLK, "rep", None), P("rep"))
    return jax.shard_map(
        shards, mesh=split, in_specs=in_specs, out_specs=out_specs, check_vma=False
    )
```

```python
import functools
import math

import jax
import jax.numpy as jnp
from jax import lax
from jax.experimental import pallas as pl
from jax.experimental.pallas import tpu as pltpu
from jax.sharding import Mesh
from jax.sharding import PartitionSpec as P


NLON = 4096
HALF = NLON // 2
BLK = ("blk_0", "blk_1", "blk_2", "blk_3")
DEPTH = 512
TILE = 256
READY = 2
ORDER = (("blk_3", 2), ("blk_2", 4), ("blk_1", 4), ("blk_0", 4))


def spectra_body(orders_hbm, cycles_hbm, coef_hbm, table_hbm, out, energy_hbm, coef, table, tail, low_sum, high_sum, onehot, moved_out, energy, orders, cycles, sems, *, slab_rows, depth):
    pairs, fields2 = coef_hbm.shape[1], coef_hbm.shape[2]
    lat = table_hbm.shape[2]
    chunks = slab_rows // depth
    whole = chunks * depth
    columns = lat // 128

    table_rows = table_hbm.reshape(slab_rows * pairs, lat)

    def piece(chunk, column):
        return pltpu.make_async_copy(
            table_rows.at[pl.ds(chunk * depth * pairs, depth * pairs), pl.ds(column * 128, 128)],
            table.at[chunk, column],
            sems.at[chunk, column],
        )

    def last(column):
        return pltpu.make_async_copy(
            table_hbm.at[pl.ds(whole, 1), :, pl.ds(column * 128, 128)],
            tail.at[column, pl.ds(0, 1)],
            sems.at[chunks, column],
        )

    coef_copy = pltpu.make_async_copy(
        coef_hbm.reshape(slab_rows * pairs, fields2), coef.at[pl.ds(0, slab_rows * pairs)], sems.at[chunks + 1, 0]
    )
    coef_copy.start()
    orders_copy = pltpu.make_async_copy(orders_hbm, orders, sems.at[chunks + 2, 0])
    orders_copy.start()
    cycles_copy = pltpu.make_async_copy(cycles_hbm, cycles, sems.at[chunks + 2, 1])
    cycles_copy.start()
    for column in range(columns):
        piece(0, column).start()
    for column in range(columns):
        last(column).start()
    for chunk in range(1, chunks):
        for column in range(columns):
            piece(chunk, column).start()

    cycles_copy.wait()
    lane = lax.broadcasted_iota(jnp.int32, (128, lat), 1)
    for at in range(0, lat, 128):
        column = jnp.broadcast_to(cycles[:, at : at + 128], (128, 128)).T
        column = jnp.concatenate([column] * columns, axis=1)
        onehot[at : at + 128, :] = (column == lane).astype(jnp.float32).astype(jnp.bfloat16)

    orders_copy.wait()
    first = lax.axis_index(BLK) * pairs
    lows = [orders[first + pair] for pair in range(pairs)]
    coef_copy.wait()

    def left_of(start, count, side):
        turned = coef[start * pairs : (start + count) * pairs, :].astype(jnp.float32).T
        lane = lax.broadcasted_iota(jnp.int32, turned.shape, 1)
        parts = []
        for pair in range(pairs):
            mine = lane % pairs == pair
            row = start + lane // pairs
            if side == "low":
                mine = mine & (row < slab_rows - 1 - lows[pair])
            elif side == "high":
                mine = mine & (row >= slab_rows - 1 - lows[pair]) & (row < slab_rows)
            parts.append(jnp.where(mine, turned, 0.0))
        return jnp.concatenate(parts, axis=0).astype(jnp.bfloat16)

    for column in range(columns):
        last(column).wait()
    ends = []
    for column in range(columns):
        end = tail.at[column].reshape(tail.shape[1] * pairs, 128)[...].astype(jnp.float32)
        keep = lax.broadcasted_iota(jnp.int32, end.shape, 0) < pairs
        ends.append(jnp.where(keep, end, 0.0).astype(jnp.bfloat16))
    ends = jnp.concatenate(ends, axis=1)
    high_sum[...] = jnp.dot(left_of(whole, tail.shape[1], "high"), ends, preferred_element_type=jnp.float32)

    for chunk in range(chunks):
        start = chunk * depth
        sure = start + depth <= slab_rows // 2
        low_left = left_of(start, depth, None if sure else "low")
        high_left = None if sure else left_of(start, depth, "high")
        for column in range(columns):
            piece(chunk, column).wait()
        right = jnp.concatenate(
            [table[chunk, column] for column in range(columns)], axis=1
        )
        low = jnp.dot(low_left, right, preferred_element_type=jnp.float32)
        low_sum[...] = low if chunk == 0 else low_sum[...] + low
        if not sure:
            high_sum[...] += jnp.dot(high_left, right, preferred_element_type=jnp.float32)

    groups, blocks, rows, _ = moved_out.shape
    slabs = out.reshape(blocks, groups * rows, fields2)
    copies = []
    lane = lax.broadcasted_iota(jnp.int32, (1, fields2), 1)
    real = lane < fields2 // 2
    total = jnp.zeros((1, fields2), jnp.float32)
    for pair in range(pairs):
        even = lows[pair] % 2 == 0
        low = low_sum[pair * fields2 : (pair + 1) * fields2, :]
        high = high_sum[pair * fields2 : (pair + 1) * fields2, :]
        spectrum = jnp.concatenate([jnp.where(even, low, high), jnp.where(even, high, low)], axis=0)
        moved = lax.dot_general(
            onehot[...],
            spectrum.astype(jnp.bfloat16),
            (((1,), (1,)), ((), ())),
            preferred_element_type=jnp.float32,
        )
        for parity in range(2):
            group = pair * 2 + parity
            part = moved[:, parity * fields2 : (parity + 1) * fields2].astype(jnp.bfloat16)
            moved_out[group] = part.reshape(blocks, rows, fields2)
            copies.append(
                pltpu.make_async_copy(
                    moved_out.at[group], slabs.at[:, pl.ds(group * rows, rows)], sems.at[chunks + 1, 1 + group]
                )
            )
            copies[-1].start()
        sums = jnp.sum(moved * moved, axis=0, keepdims=True)
        weight = jnp.where(lows[pair] == 0, jnp.where(real, 1.0, 0.0), 2.0)
        total = total + sums[:, :fields2] * weight + sums[:, fields2:] * 2.0
    total = (total + pltpu.roll(total, fields2 // 2, 1)) * (1.0 / lat)
    energy[...] = total
    copies.append(pltpu.make_async_copy(energy, energy_hbm, sems.at[chunks + 2, 2]))
    copies[-1].start()
    for copy in copies:
        copy.wait()


def spectra_of(load_coef, legendre, slab_orders, cycle_rows, blocks):
    pairs, slab_rows, fields2 = load_coef.shape
    lat = legendre.shape[2]
    columns = lat // 128
    chunks = slab_rows // DEPTH
    tiles = lat // blocks // 2
    anywhere = pl.BlockSpec(memory_space=pltpu.HBM)
    return pl.pallas_call(
        functools.partial(spectra_body, slab_rows=slab_rows, depth=DEPTH),
        in_specs=[anywhere] * 4,
        out_specs=[anywhere, anywhere],
        out_shape=[
            jax.ShapeDtypeStruct((blocks, pairs * 2 * tiles, 2, fields2), jnp.bfloat16),
            jax.ShapeDtypeStruct((1, fields2), jnp.float32),
        ],
        scratch_shapes=[
            pltpu.VMEM(((slab_rows // 64 * 64 + 64) * pairs, fields2), jnp.bfloat16),
            pltpu.VMEM((chunks, columns, DEPTH * pairs, 128), jnp.bfloat16),
            pltpu.VMEM((columns, 8, pairs, 128), jnp.bfloat16),
            pltpu.VMEM((pairs * fields2, lat), jnp.float32),
            pltpu.VMEM((pairs * fields2, lat), jnp.float32),
            pltpu.VMEM((lat, lat), jnp.bfloat16),
            pltpu.VMEM((pairs * 2, blocks, tiles * 2, fields2), jnp.bfloat16),
            pltpu.VMEM((1, fields2), jnp.float32),
            pltpu.SMEM(slab_orders.shape, jnp.int32),
            pltpu.VMEM((1, lat), jnp.int32),
            pltpu.SemaphoreType.DMA((chunks + 3, columns)),
        ],
        compiler_params=pltpu.CompilerParams(vmem_limit_bytes=60 * 2**20),
        name="spectra",
    )(slab_orders, cycle_rows.reshape(1, lat), jnp.transpose(load_coef, (1, 0, 2)), jnp.transpose(legendre, (1, 0, 2)))


def angles_body(orders, out, ready, columns, *, pairs, blocks, degree):
    count = pairs * blocks
    columns[...] = jnp.broadcast_to(orders[...], (128, count)).T
    lane = lax.broadcasted_iota(jnp.int32, (blocks, 128), 1)
    scale = 2.0 * math.pi / NLON
    for pair in range(pairs):
        low = columns[pl.ds(pair, blocks, stride=pairs), :]
        high = degree - low
        is_even = low % 2 == 0
        for parity, order in enumerate((jnp.where(is_even, low, high), jnp.where(is_even, high, low))):
            fine = (order * lane % NLON).astype(jnp.float32) * scale
            turn = (order * 128 % NLON).astype(jnp.float32) * scale
            factor = jnp.where(order == 0, 1.0, 2.0)
            at = pl.ds(pair * blocks, blocks)
            cosine, sine = factor * jnp.cos(fine), -factor * jnp.sin(fine)
            turn_cos, turn_sin = jnp.cos(turn), jnp.sin(turn)
            for lane_at in range(0, READY * TILE, 128):
                tile, to = lane_at // TILE, slice(lane_at % TILE, lane_at % TILE + 128)
                ready[tile, parity, pl.ds(2 * pair * blocks, blocks), to] = cosine.astype(jnp.bfloat16)
                ready[tile, parity, pl.ds((2 * pair + 1) * blocks, blocks), to] = sine.astype(jnp.bfloat16)
                cosine, sine = cosine * turn_cos + sine * turn_sin, sine * turn_cos - cosine * turn_sin
            out[parity, 0, at, :] = cosine
            out[parity, 1, at, :] = sine
            out[parity, 2, at, :] = turn_cos
            out[parity, 3, at, :] = turn_sin


def angles_of(slab_orders, pairs, blocks, degree):
    return pl.pallas_call(
        functools.partial(angles_body, pairs=pairs, blocks=blocks, degree=degree),
        in_specs=[pl.BlockSpec(memory_space=pltpu.VMEM)],
        out_specs=[pl.BlockSpec(memory_space=pltpu.VMEM)] * 2,
        out_shape=[
            jax.ShapeDtypeStruct((2, 4, pairs * blocks, 128), jnp.float32),
            jax.ShapeDtypeStruct((READY, 2, 2 * pairs * blocks, TILE), jnp.bfloat16),
        ],
        scratch_shapes=[pltpu.VMEM((pairs * blocks, 128), jnp.int32)],
        compiler_params=pltpu.CompilerParams(vmem_limit_bytes=12 * 2**20),
        name="angles",
    )(slab_orders.reshape(1, pairs * blocks))


def wave_body(received, angles, ready, out, slabs, wide, state, lefts, basis, staged, sems, *, pairs, blocks, rows, fields):
    tiles = HALF // TILE
    stride = wide.shape[1]
    slabs_copy = pltpu.make_async_copy(received.reshape(*slabs.shape), slabs, sems.at[2, 1])
    slabs_copy.start()

    def build(tile):
        for parity in range(2):
            for pair in range(pairs):
                at = pl.ds(pair * blocks, blocks)
                held = angles if tile == READY else state
                cosine, sine = held[parity, 0, at, :], held[parity, 1, at, :]
                turn_cos, turn_sin = angles[parity, 2, at, :], angles[parity, 3, at, :]
                for lane in range(0, TILE, 128):
                    to = slice(lane, lane + 128)
                    basis[tile - READY, parity, pl.ds(2 * pair * blocks, blocks), to] = cosine.astype(jnp.bfloat16)
                    basis[tile - READY, parity, pl.ds((2 * pair + 1) * blocks, blocks), to] = sine.astype(jnp.bfloat16)
                    cosine, sine = cosine * turn_cos + sine * turn_sin, sine * turn_cos - cosine * turn_sin
                state[parity, 0, at, :] = cosine
                state[parity, 1, at, :] = sine

    slabs_copy.wait()
    per_slab = slabs.shape[0] // blocks
    wide[:, :per_slab, :] = slabs[...].astype(jnp.float32).reshape(blocks, per_slab, slabs.shape[1])
    spaced = wide.reshape(blocks * stride, slabs.shape[1])
    for pair in range(pairs):
        for parity in range(2):
            for row in range(rows):
                at = (pair * 2 + parity) * rows + row
                turned = spaced[pl.ds(at, blocks, stride=stride), :].T.astype(jnp.bfloat16)
                for part in range(2):
                    to = (pair * 2 + part) * blocks
                    lefts[parity, row * fields : (row + 1) * fields, to : to + blocks] = turned[
                        part * fields : (part + 1) * fields, :
                    ]

    def copy(half, tile):
        at = half * HALF + tile * TILE
        return pltpu.make_async_copy(
            staged.at[:, :, pl.ds(at, TILE)], out.at[:, :, pl.ds(at, TILE)], sems.at[half, tile]
        )

    for tile in range(tiles):
        at = tile * TILE
        right = ready.at[tile] if tile < READY else basis.at[tile - READY]
        even = jnp.dot(lefts[0], right[0], preferred_element_type=jnp.float32)
        odd = jnp.dot(lefts[1], right[1], preferred_element_type=jnp.float32)
        if READY <= tile + 1 < tiles:
            build(tile + 1)
        for half, value in enumerate((even + odd, even - odd)):
            to = half * HALF + at
            staged[:, :, to : to + TILE] = value.astype(jnp.bfloat16).reshape(rows, fields, TILE)
            copy(half, tile).start()

    for tile in range(tiles):
        for half in range(2):
            copy(half, tile).wait()


def wave_of(received, angles, pairs, blocks, rows, fields):
    depth = 2 * pairs * blocks
    tiles = HALF // TILE
    anywhere = pl.BlockSpec(memory_space=pl.ANY)
    flat = (received.size // (2 * fields), 2 * fields)
    return pl.pallas_call(
        functools.partial(wave_body, pairs=pairs, blocks=blocks, rows=rows, fields=fields),
        in_specs=[anywhere, pl.BlockSpec(memory_space=pltpu.VMEM), pl.BlockSpec(memory_space=pltpu.VMEM)],
        out_specs=pl.BlockSpec(memory_space=pltpu.HBM),
        out_shape=jax.ShapeDtypeStruct((rows, fields, NLON), jnp.bfloat16),
        scratch_shapes=[
            pltpu.VMEM(flat, jnp.bfloat16),
            pltpu.VMEM((blocks, flat[0] // blocks + 8, flat[1]), jnp.float32),
            pltpu.VMEM((2, 2, *angles[0].shape[2:]), jnp.float32),
            pltpu.VMEM((2, rows * fields, depth), jnp.bfloat16),
            pltpu.VMEM((tiles - READY, 2, depth, TILE), jnp.bfloat16),
            pltpu.VMEM((rows, fields, NLON), jnp.bfloat16),
            pltpu.SemaphoreType.DMA((3, tiles)),
        ],
        compiler_params=pltpu.CompilerParams(vmem_limit_bytes=24 * 2**20),
        name="wave",
    )(received, *angles)


def shards(load_coef, legendre, slab_orders, cycle_rows):
    blocks = lax.axis_size(BLK)
    pairs, slab_rows, fields2 = load_coef.shape
    lat = legendre.shape[2]
    rows = lat // blocks
    spectra, energy = spectra_of(load_coef, legendre, slab_orders, cycle_rows, blocks)
    received = lax.all_to_all(spectra, BLK, split_axis=0, concat_axis=0, tiled=True)
    angles = angles_of(slab_orders, pairs, blocks, slab_rows - 2)
    for axis, size in ORDER:
        other = [
            lax.ppermute(energy, axis, [(at, at ^ step) for at in range(size)]) for step in range(1, size)
        ]
        energy = energy + other[0]
        if size == 4:
            energy = energy + (other[1] + other[2])
    wave = wave_of(received, angles, pairs, blocks, rows, fields2 // 2)
    return wave, energy[0, : fields2 // 2]


def solution(mesh):
    split = Mesh(
        mesh.devices.reshape(4, 4, 4, 2, mesh.shape["rep"]),
        ("blk_0", "blk_1", "blk_2", "blk_3", "rep"),
    )
    in_specs = (P(BLK, None, "rep"), P(BLK, None, None), P(), P())
    out_specs = (P(BLK, "rep", None), P("rep"))
    return jax.shard_map(
        shards, mesh=split, in_specs=in_specs, out_specs=out_specs, check_vma=False
    )
```

```python
import functools
import math

import jax
import jax.numpy as jnp
from jax import lax
from jax.experimental import pallas as pl
from jax.experimental.pallas import tpu as pltpu
from jax.sharding import Mesh
from jax.sharding import PartitionSpec as P


NLON = 4096
HALF = NLON // 2
BLK = ("blk_0", "blk_1", "blk_2", "blk_3")
DEPTH = 512
TILE = 512
READY = 1
ORDER = (("blk_3", 2), ("blk_2", 4), ("blk_1", 4), ("blk_0", 4))


def spectra_body(orders_hbm, cycles_hbm, coef_hbm, table_hbm, out, energy_hbm, coef, table, tail, low_sum, high_sum, moved_out, energy, orders, cycles, sems, *, slab_rows, depth):
    pairs, fields2 = coef_hbm.shape[1], coef_hbm.shape[2]
    lat = table_hbm.shape[2]
    chunks = slab_rows // depth
    whole = chunks * depth
    columns = lat // 128

    table_rows = table_hbm.reshape(slab_rows * pairs, lat)

    def piece(chunk, column):
        return pltpu.make_async_copy(
            table_rows.at[pl.ds(chunk * depth * pairs, depth * pairs), pl.ds(column * 128, 128)],
            table.at[chunk, column],
            sems.at[chunk, column],
        )

    def last(column):
        return pltpu.make_async_copy(
            table_hbm.at[pl.ds(whole, 1), :, pl.ds(column * 128, 128)],
            tail.at[column, pl.ds(0, 1)],
            sems.at[chunks, column],
        )

    coef_copy = pltpu.make_async_copy(
        coef_hbm.reshape(slab_rows * pairs, fields2), coef.at[pl.ds(0, slab_rows * pairs)], sems.at[chunks + 1, 0]
    )
    coef_copy.start()
    orders_copy = pltpu.make_async_copy(orders_hbm, orders, sems.at[chunks + 2, 0])
    orders_copy.start()
    cycles_copy = pltpu.make_async_copy(cycles_hbm, cycles, sems.at[chunks + 2, 1])
    cycles_copy.start()
    for column in range(columns):
        piece(0, column).start()
    for column in range(columns):
        last(column).start()
    for chunk in range(1, chunks):
        for column in range(columns):
            piece(chunk, column).start()

    orders_copy.wait()
    cycles_copy.wait()
    first = lax.axis_index(BLK) * pairs
    lows = [orders[first + pair] for pair in range(pairs)]
    coef_copy.wait()

    def left_of(start, count, side):
        turned = coef[start * pairs : (start + count) * pairs, :].astype(jnp.float32).T
        lane = lax.broadcasted_iota(jnp.int32, turned.shape, 1)
        parts = []
        for pair in range(pairs):
            mine = lane % pairs == pair
            row = start + lane // pairs
            if side == "low":
                mine = mine & (row < slab_rows - 1 - lows[pair])
            elif side == "high":
                mine = mine & (row >= slab_rows - 1 - lows[pair]) & (row < slab_rows)
            parts.append(jnp.where(mine, turned, 0.0))
        return jnp.concatenate(parts, axis=0).astype(jnp.bfloat16)

    for column in range(columns):
        last(column).wait()
    ends = []
    for column in range(columns):
        end = tail.at[column].reshape(tail.shape[1] * pairs, 128)[...].astype(jnp.float32)
        keep = lax.broadcasted_iota(jnp.int32, end.shape, 0) < pairs
        ends.append(jnp.where(keep, end, 0.0).astype(jnp.bfloat16))
    ends = jnp.concatenate(ends, axis=1)
    high_sum[...] = jnp.dot(left_of(whole, tail.shape[1], "high"), ends, preferred_element_type=jnp.float32)

    for chunk in range(chunks):
        start = chunk * depth
        sure = start + depth <= slab_rows // 2
        low_left = left_of(start, depth, None if sure else "low")
        high_left = None if sure else left_of(start, depth, "high")
        for column in range(columns):
            piece(chunk, column).wait()
        right = jnp.concatenate(
            [table[chunk, column] for column in range(columns)], axis=1
        )
        low = jnp.dot(low_left, right, preferred_element_type=jnp.float32)
        low_sum[...] = low if chunk == 0 else low_sum[...] + low
        if not sure:
            high_sum[...] += jnp.dot(high_left, right, preferred_element_type=jnp.float32)

    spectrum = []
    for pair in range(pairs):
        even = lows[pair] % 2 == 0
        low = low_sum[pair * fields2 : (pair + 1) * fields2, :]
        high = high_sum[pair * fields2 : (pair + 1) * fields2, :]
        spectrum.append(jnp.where(even, low, high).astype(jnp.bfloat16))
        spectrum.append(jnp.where(even, high, low).astype(jnp.bfloat16))
    spectrum = jnp.concatenate(spectrum, axis=0)

    lane = lax.broadcasted_iota(jnp.int32, (128, lat), 1)
    onehot = []
    for at in range(0, lat, 128):
        column = jnp.broadcast_to(cycles[:, at : at + 128], (128, 128)).T
        column = jnp.concatenate([column] * columns, axis=1)
        onehot.append((column == lane).astype(jnp.float32).astype(jnp.bfloat16))
    onehot = jnp.concatenate(onehot, axis=0)
    moved = lax.dot_general(onehot, spectrum, (((1,), (1,)), ((), ())), preferred_element_type=jnp.float32)
    groups, blocks, rows, _ = moved_out.shape
    slabs = out.reshape(blocks, groups * rows, fields2)
    copies = []
    for group in range(groups):
        part = moved[:, group * fields2 : (group + 1) * fields2].astype(jnp.bfloat16)
        moved_out[group] = part.reshape(blocks, rows, fields2)
        copies.append(
            pltpu.make_async_copy(
                moved_out.at[group], slabs.at[:, pl.ds(group * rows, rows)], sems.at[chunks + 1, 1 + group]
            )
        )
        copies[-1].start()

    sums = jnp.sum(moved * moved, axis=0, keepdims=True)
    lane = lax.broadcasted_iota(jnp.int32, (1, fields2), 1)
    real = lane < fields2 // 2
    total = jnp.zeros((1, fields2), jnp.float32)
    for pair in range(pairs):
        weight = jnp.where(lows[pair] == 0, jnp.where(real, 1.0, 0.0), 2.0)
        at = 2 * pair * fields2
        total = total + sums[:, at : at + fields2] * weight + sums[:, at + fields2 : at + 2 * fields2] * 2.0
    total = (total + pltpu.roll(total, fields2 // 2, 1)) * (1.0 / lat)
    energy[...] = total
    copies.append(pltpu.make_async_copy(energy, energy_hbm, sems.at[chunks + 2, 2]))
    copies[-1].start()
    for copy in copies:
        copy.wait()


def spectra_of(load_coef, legendre, slab_orders, cycle_rows, blocks):
    pairs, slab_rows, fields2 = load_coef.shape
    lat = legendre.shape[2]
    columns = lat // 128
    chunks = slab_rows // DEPTH
    tiles = lat // blocks // 2
    anywhere = pl.BlockSpec(memory_space=pltpu.HBM)
    return pl.pallas_call(
        functools.partial(spectra_body, slab_rows=slab_rows, depth=DEPTH),
        in_specs=[anywhere] * 4,
        out_specs=[anywhere, anywhere],
        out_shape=[
            jax.ShapeDtypeStruct((blocks, pairs * 2 * tiles, 2, fields2), jnp.bfloat16),
            jax.ShapeDtypeStruct((1, fields2), jnp.float32),
        ],
        scratch_shapes=[
            pltpu.VMEM(((slab_rows // 64 * 64 + 64) * pairs, fields2), jnp.bfloat16),
            pltpu.VMEM((chunks, columns, DEPTH * pairs, 128), jnp.bfloat16),
            pltpu.VMEM((columns, 8, pairs, 128), jnp.bfloat16),
            pltpu.VMEM((pairs * fields2, lat), jnp.float32),
            pltpu.VMEM((pairs * fields2, lat), jnp.float32),
            pltpu.VMEM((pairs * 2, blocks, tiles * 2, fields2), jnp.bfloat16),
            pltpu.VMEM((1, fields2), jnp.float32),
            pltpu.SMEM(slab_orders.shape, jnp.int32),
            pltpu.VMEM((1, lat), jnp.int32),
            pltpu.SemaphoreType.DMA((chunks + 3, columns)),
        ],
        compiler_params=pltpu.CompilerParams(vmem_limit_bytes=60 * 2**20),
        name="spectra",
    )(slab_orders, cycle_rows.reshape(1, lat), jnp.transpose(load_coef, (1, 0, 2)), jnp.transpose(legendre, (1, 0, 2)))


def angles_body(orders, out, ready, columns, *, pairs, blocks, degree):
    count = pairs * blocks
    columns[...] = jnp.broadcast_to(orders[...], (128, count)).T
    lane = lax.broadcasted_iota(jnp.int32, (blocks, 128), 1)
    scale = 2.0 * math.pi / NLON
    for pair in range(pairs):
        low = columns[pl.ds(pair, blocks, stride=pairs), :]
        high = degree - low
        is_even = low % 2 == 0
        for parity, order in enumerate((jnp.where(is_even, low, high), jnp.where(is_even, high, low))):
            fine = (order * lane % NLON).astype(jnp.float32) * scale
            turn = (order * 128 % NLON).astype(jnp.float32) * scale
            factor = jnp.where(order == 0, 1.0, 2.0)
            at = pl.ds(pair * blocks, blocks)
            cosine, sine = factor * jnp.cos(fine), -factor * jnp.sin(fine)
            turn_cos, turn_sin = jnp.cos(turn), jnp.sin(turn)
            for lane_at in range(0, READY * TILE, 128):
                tile, to = lane_at // TILE, slice(lane_at % TILE, lane_at % TILE + 128)
                ready[tile, parity, pl.ds(2 * pair * blocks, blocks), to] = cosine.astype(jnp.bfloat16)
                ready[tile, parity, pl.ds((2 * pair + 1) * blocks, blocks), to] = sine.astype(jnp.bfloat16)
                cosine, sine = cosine * turn_cos + sine * turn_sin, sine * turn_cos - cosine * turn_sin
            out[parity, 0, at, :] = cosine
            out[parity, 1, at, :] = sine
            out[parity, 2, at, :] = turn_cos
            out[parity, 3, at, :] = turn_sin


def angles_of(slab_orders, pairs, blocks, degree):
    return pl.pallas_call(
        functools.partial(angles_body, pairs=pairs, blocks=blocks, degree=degree),
        in_specs=[pl.BlockSpec(memory_space=pltpu.VMEM)],
        out_specs=[pl.BlockSpec(memory_space=pltpu.VMEM)] * 2,
        out_shape=[
            jax.ShapeDtypeStruct((2, 4, pairs * blocks, 128), jnp.float32),
            jax.ShapeDtypeStruct((READY, 2, 2 * pairs * blocks, TILE), jnp.bfloat16),
        ],
        scratch_shapes=[pltpu.VMEM((pairs * blocks, 128), jnp.int32)],
        compiler_params=pltpu.CompilerParams(vmem_limit_bytes=12 * 2**20),
        name="angles",
    )(slab_orders.reshape(1, pairs * blocks))


def wave_body(received, angles, ready, out, slabs, wide, state, lefts, basis, staged, sems, *, pairs, blocks, rows, fields):
    tiles = HALF // TILE
    stride = wide.shape[1]
    slabs_copy = pltpu.make_async_copy(received.reshape(*slabs.shape), slabs, sems.at[2, 1])
    slabs_copy.start()

    def build(tile):
        for parity in range(2):
            for pair in range(pairs):
                at = pl.ds(pair * blocks, blocks)
                held = angles if tile == READY else state
                cosine, sine = held[parity, 0, at, :], held[parity, 1, at, :]
                turn_cos, turn_sin = angles[parity, 2, at, :], angles[parity, 3, at, :]
                for lane in range(0, TILE, 128):
                    to = slice(lane, lane + 128)
                    basis[tile - READY, parity, pl.ds(2 * pair * blocks, blocks), to] = cosine.astype(jnp.bfloat16)
                    basis[tile - READY, parity, pl.ds((2 * pair + 1) * blocks, blocks), to] = sine.astype(jnp.bfloat16)
                    cosine, sine = cosine * turn_cos + sine * turn_sin, sine * turn_cos - cosine * turn_sin
                state[parity, 0, at, :] = cosine
                state[parity, 1, at, :] = sine

    slabs_copy.wait()
    per_slab = slabs.shape[0] // blocks
    wide[:, :per_slab, :] = slabs[...].astype(jnp.float32).reshape(blocks, per_slab, slabs.shape[1])
    spaced = wide.reshape(blocks * stride, slabs.shape[1])
    for pair in range(pairs):
        for parity in range(2):
            for row in range(rows):
                at = (pair * 2 + parity) * rows + row
                turned = spaced[pl.ds(at, blocks, stride=stride), :].T.astype(jnp.bfloat16)
                for part in range(2):
                    to = (pair * 2 + part) * blocks
                    lefts[parity, row * fields : (row + 1) * fields, to : to + blocks] = turned[
                        part * fields : (part + 1) * fields, :
                    ]

    def copy(half, tile):
        at = half * HALF + tile * TILE
        return pltpu.make_async_copy(
            staged.at[:, :, pl.ds(at, TILE)], out.at[:, :, pl.ds(at, TILE)], sems.at[half, tile]
        )

    for tile in range(tiles):
        at = tile * TILE
        right = ready.at[tile] if tile < READY else basis.at[tile - READY]
        even = jnp.dot(lefts[0], right[0], preferred_element_type=jnp.float32)
        odd = jnp.dot(lefts[1], right[1], preferred_element_type=jnp.float32)
        if READY <= tile + 1 < tiles:
            build(tile + 1)
        for half, value in enumerate((even + odd, even - odd)):
            to = half * HALF + at
            staged[:, :, to : to + TILE] = value.astype(jnp.bfloat16).reshape(rows, fields, TILE)
            copy(half, tile).start()

    for tile in range(tiles):
        for half in range(2):
            copy(half, tile).wait()


def wave_of(received, angles, pairs, blocks, rows, fields):
    depth = 2 * pairs * blocks
    tiles = HALF // TILE
    anywhere = pl.BlockSpec(memory_space=pl.ANY)
    flat = (received.size // (2 * fields), 2 * fields)
    return pl.pallas_call(
        functools.partial(wave_body, pairs=pairs, blocks=blocks, rows=rows, fields=fields),
        in_specs=[anywhere, pl.BlockSpec(memory_space=pltpu.VMEM), pl.BlockSpec(memory_space=pltpu.VMEM)],
        out_specs=pl.BlockSpec(memory_space=pltpu.HBM),
        out_shape=jax.ShapeDtypeStruct((rows, fields, NLON), jnp.bfloat16),
        scratch_shapes=[
            pltpu.VMEM(flat, jnp.bfloat16),
            pltpu.VMEM((blocks, flat[0] // blocks + 8, flat[1]), jnp.float32),
            pltpu.VMEM((2, 2, *angles[0].shape[2:]), jnp.float32),
            pltpu.VMEM((2, rows * fields, depth), jnp.bfloat16),
            pltpu.VMEM((tiles - READY, 2, depth, TILE), jnp.bfloat16),
            pltpu.VMEM((rows, fields, NLON), jnp.bfloat16),
            pltpu.SemaphoreType.DMA((3, tiles)),
        ],
        compiler_params=pltpu.CompilerParams(vmem_limit_bytes=24 * 2**20),
        name="wave",
    )(received, *angles)


def shards(load_coef, legendre, slab_orders, cycle_rows):
    blocks = lax.axis_size(BLK)
    pairs, slab_rows, fields2 = load_coef.shape
    lat = legendre.shape[2]
    rows = lat // blocks
    spectra, energy = spectra_of(load_coef, legendre, slab_orders, cycle_rows, blocks)
    received = lax.all_to_all(spectra, BLK, split_axis=0, concat_axis=0, tiled=True)
    angles = angles_of(slab_orders, pairs, blocks, slab_rows - 2)
    for axis, size in ORDER:
        other = [
            lax.ppermute(energy, axis, [(at, at ^ step) for at in range(size)]) for step in range(1, size)
        ]
        energy = energy + other[0]
        if size == 4:
            energy = energy + (other[1] + other[2])
    wave = wave_of(received, angles, pairs, blocks, rows, fields2 // 2)
    return wave, energy[0, : fields2 // 2]


def solution(mesh):
    split = Mesh(
        mesh.devices.reshape(4, 4, 4, 2, mesh.shape["rep"]),
        ("blk_0", "blk_1", "blk_2", "blk_3", "rep"),
    )
    in_specs = (P(BLK, None, "rep"), P(BLK, None, None), P(), P())
    out_specs = (P(BLK, "rep", None), P("rep"))
    return jax.shard_map(
        shards, mesh=split, in_specs=in_specs, out_specs=out_specs, check_vma=False
    )
```
